32 devices in a mesh: span: 8 (over z, y), depth: 4 (over x, core).
Axes of the slice: x: 2, y: 2, z: 4, core: 2. Of those that a mesh axis runs over, the one named last changes fastest.
Arguments:
- part_slab: int32 [4, 65536, 1], P('depth', 'span'), may hold values from 0 to 7; in each aligned block of 8192 rows (0 to 8191, 8192 to 16383, ..., all dimensions but the last counted through in order) at most 2048 rows name the same one
- part_cell: int32 [4, 65536], P('depth', 'span'), may hold values from 0 to 65535
- part_volume: float32 [4, 65536], P('depth', 'span'), may hold values from 0.05 to 0.6
- part_drag: float32 [3, 4, 65536], P(None, 'depth', 'span'), may hold values from -6 to 6
- part_count: int32 [4, 8], P('depth', 'span'), may hold values from 7168 to 8192
- prior_solid: float32 [8, 128, 2048], P(None, 'span', 'depth'), may hold values from 0 to 0.6
- prior_drag: float32 [3, 8, 128, 2048], P(None, None, 'span', 'depth'), may hold values from -4 to 4
Outputs:
- fields: float32 [4, 8, 128, 2048], P(None, None, 'span', 'depth')
- feedback: float32 [4, 4, 65536], P(None, 'depth', 'span')
The draws below stay inside these ranges and needn't reach their ends.
Inputs may be any that keep to these rules, and one draw needn't show every extreme that they name: `part_slab`: among the 8192 particle slots of one owner device, live or not, no slab is named more than 2048 times; in every draw some device names a slab exactly 2048 times.
All inputs are finite; a program needn't handle non-finite values.
Results may differ from the reference program's by a relative error of at most 0.0003.
Values sent between devices are 32-bit elements; how exact they have to be, the bound alone decides.
A program may use at most 128 MiB of HBM per device.

```python
import math
import jax
import jax.numpy as jnp
import numpy as np

CX = 16
CY = 512
LAYERS = 8
SWEEPS = 6
PART_DEV = 8192
CAP = 2048
NX = 128
NY = 2048
SPAN_PARTS = 65536
N_SPAN = 8
N_DEPTH = 4


def with_ends(entries, own_key, low, top_value):
    spot = [jax.random.randint(jax.random.fold_in(own_key, axis), (), 0, length) for axis, length in enumerate(entries.shape)]
    longest = entries.shape.index(max(entries.shape))
    next_to = spot[:longest] + [(spot[longest] + 1) % entries.shape[longest]] + spot[longest + 1:]
    return entries.at[tuple(spot)].set(low).at[tuple(next_to)].set(top_value)


def levels(stream_key, extent, split, least, high):
    factor_of, own = 1.0, jax.random.fold_in(stream_key, 6)
    for axis_at, shards_of in split:
        draws = jnp.exp(jax.random.uniform(jax.random.fold_in(own, axis_at), (shards_of,), jnp.float32, least / len(split), high / len(split)))
        factor_of = factor_of * jnp.repeat(draws, extent[axis_at] // shards_of).reshape([-1 if axis == axis_at else 1 for axis in range(len(extent))])
    return factor_of


def deal_out(key, own, number, rows, number_of, top, most, skew):
    ranking = jax.random.permutation(key, number_of)
    crowded, usual = portions_of(number_of, rows * top, most, skew, True), portions_of(number_of, rows * top, most, skew, False)
    places = jnp.arange(number_of)

    def named(lengths, rotation):
        used = int((lengths > 0).sum())
        fixed = max(1, used // 4)
        passed = fixed + (places - fixed + rotation * (used - fixed)) % max(1, number_of - fixed)
        return jnp.zeros((number_of,), jnp.int32).at[ranking[jnp.where(places < fixed, places, passed)]].set(jnp.asarray(lengths, jnp.int32))

    lengths = jnp.where(number % 4 == 0, named(crowded, number // 4), named(usual, number - number // 4 - 1))
    mixed = jax.random.permutation(jax.random.fold_in(own, 3), number_of)
    giver, receiver = mixed[0:number_of // 2 * 2:2], mixed[1:number_of // 2 * 2:2]
    room = jnp.minimum(lengths[giver] - 1, most - lengths[receiver]) // 2
    room = jnp.where((giver == ranking[0]) | (receiver == ranking[0]) | (lengths[receiver] == 0), 0, jnp.maximum(room, 0))
    passed = jax.random.randint(jax.random.fold_in(own, 4), (number_of // 2,), 0, 1 << 20) % (room + 1)
    lengths = lengths.at[giver].add(-passed).at[receiver].add(passed)
    labels = jnp.searchsorted(jnp.cumsum(lengths), jnp.arange(rows * top), side="right").astype(jnp.int32)
    table = labels.reshape(top, rows).T
    table = table[jax.random.permutation(jax.random.fold_in(own, 1), rows)]
    rotation = jax.random.randint(jax.random.fold_in(own, 2), (rows, 1), 0, top)
    return jnp.take_along_axis(table, (jnp.arange(top)[None, :] + rotation) % top, axis=1)


def portions_of(number_of, total, most, lean, full):
    portions = [(1 << 20) // math.isqrt(grade ** lean) + 1 for grade in range(1, number_of + 1)]
    largest = most if full else min(most, max(-(-total // number_of), total * portions[0] // sum(portions)))
    least = 1 if total - largest >= number_of - 1 else 0
    holding, rest = [largest] + [least] * (number_of - 1), total - largest - least * (number_of - 1)
    while rest > 0:
        free = [i for i in range(1, number_of) if holding[i] < largest] or [i for i in range(1, number_of) if holding[i] < most]
        mass, remaining = sum([portions[i] for i in free]), rest
        for i in free:
            more = min(most - holding[i], max(1, remaining * portions[i] // mass), rest)
            holding[i] = holding[i] + more
            rest = rest - more
    return np.array(holding)


def normal_values(stream_key, dims, scale, bound, pieces=(), held_as=jnp.bfloat16):
    values = jax.random.normal(stream_key, dims, jnp.float32) * scale
    if len(pieces) > 0:
        values = levels(stream_key, dims, pieces, -0.22, 0.18) * values
    return jnp.clip(values, min=-bound, max=bound).astype(held_as)


def setup_inputs(seed: int = 0) -> dict:
    key_of = jax.random.split(jax.random.key(seed), 8)
    part_slab_keys = jax.random.split(jax.random.fold_in(key_of[0], 1), N_DEPTH * SPAN_PARTS // PART_DEV)
    part_slab_turns = jax.random.permutation(jax.random.fold_in(key_of[0], 3), N_DEPTH * SPAN_PARTS // PART_DEV)
    part_slab = jax.vmap(lambda own, number: deal_out(jax.random.fold_in(key_of[0], 2), own, number, PART_DEV, N_SPAN, 1, CAP, 2))(part_slab_keys, part_slab_turns).reshape((N_DEPTH, SPAN_PARTS, 1))
    part_cell = with_ends(jax.random.randint(key_of[1], (N_DEPTH, SPAN_PARTS), 0, LAYERS * CX * CY), jax.random.fold_in(key_of[1], 1), 0, (LAYERS * CX * CY) - 1).astype(jnp.int32)
    part_volume = jnp.clip(jnp.exp(math.log(0.6) - 2.4849067 * jax.random.uniform(key_of[2], (N_DEPTH, SPAN_PARTS), jnp.float32) ** levels(key_of[2], (N_DEPTH, SPAN_PARTS), ((0, 4), (1, 8)), -0.2, 0.2)), 0.05, 0.6)
    part_drag = normal_values(key_of[3], (3, N_DEPTH, SPAN_PARTS), 1.0, 6.0, ((1, 4), (2, 8)), jnp.float32)
    part_count = with_ends(jax.random.randint(key_of[4], (N_DEPTH, N_SPAN), PART_DEV * 7 // 8, PART_DEV + 1), jax.random.fold_in(key_of[4], 1), PART_DEV * 7 // 8, PART_DEV).astype(jnp.int32)
    prior_solid = jnp.clip(0.6 * jax.random.uniform(key_of[5], (LAYERS, NX, NY), jnp.float32) ** levels(key_of[5], (LAYERS, NX, NY), ((1, 8), (2, 4)), -0.2, 0.2), 0.0, 0.6)
    prior_drag = normal_values(key_of[6], (3, LAYERS, NX, NY), 0.5, 4.0, ((2, 8), (3, 4)), jnp.float32)
    return dict(part_slab=part_slab, part_cell=part_cell, part_volume=part_volume, part_drag=part_drag, part_count=part_count, prior_solid=prior_solid, prior_drag=prior_drag)


NU_WEIGHT = 1.0
PHI_LIMIT = 0.6


def relax_once(source, padded):
    beside = padded[:, :, 2:, 1:-1] + padded[:, :, :-2, 1:-1]
    beside = beside + padded[:, :, 1:-1, 2:] + padded[:, :, 1:-1, :-2]
    return (source + NU_WEIGHT * beside) / (1.0 + 4.0 * NU_WEIGHT)


def reference(part_slab, part_cell, part_volume, part_drag, part_count, prior_solid, prior_drag):
    depth_count = part_cell.shape[0]
    span_rows = part_cell.shape[1]
    grid_x = CX * N_SPAN
    grid_y = CY * N_DEPTH
    slab_index = part_slab[:, :, 0]
    column = jnp.arange(span_rows, dtype=jnp.int32)
    owner_index = column // PART_DEV
    within = column % PART_DEV
    counts = part_count[:, owner_index]
    live_weight = (within[None, :] < counts).astype(jnp.float32)
    layer_index = part_cell // (CX * CY)
    local_x = (part_cell // CY) % CX
    local_y = part_cell % CY
    depth_row = jnp.arange(depth_count, dtype=jnp.int32)[:, None]
    flat_index = layer_index * (grid_x * grid_y) + (slab_index * CX + local_x) * grid_y + depth_row * CY + local_y
    flat_index = flat_index.astype(jnp.int32).reshape(-1)
    payload = jnp.concatenate([part_volume[None], part_drag], axis=0) * live_weight[None]
    deposit = jax.ops.segment_sum(payload.reshape(4, -1).T, flat_index, num_segments=LAYERS * grid_x * grid_y)
    deposit = deposit.T.reshape(4, LAYERS, grid_x, grid_y)
    target = jnp.concatenate([jnp.minimum(deposit[:1], PHI_LIMIT), deposit[1:]], axis=0)
    smooth = jnp.concatenate([prior_solid[None], prior_drag], axis=0)
    for sweep_index in range(SWEEPS):
        padded = jnp.pad(smooth, ((0, 0), (0, 0), (1, 1), (1, 1)))
        smooth = relax_once(target, padded)
    void_fraction = 1.0 - smooth[0]
    fields = jnp.concatenate([void_fraction[None], -smooth[1:] / void_fraction[None]], axis=0)
    feedback = fields.reshape(4, -1)[:, flat_index].reshape(4, depth_count, span_rows) * live_weight[None]
    return (fields, feedback)
```

```python
import functools
import math

import jax
import jax.numpy as jnp
from jax import lax
from jax.experimental import pallas as pl
from jax.experimental.pallas import tpu as pltpu
from jax.sharding import PartitionSpec as P

SWEEPS = 6
NU_WEIGHT = 1.0
PHI_LIMIT = 0.6
BF = jnp.bfloat16
F32 = jnp.float32


def two_parts(value):
    high = value.astype(BF)
    return high, (value - high.astype(F32)).astype(BF)


def nt_dot(left, right):
    return lax.dot_general(left, right, (((1,), (1,)), ((), ())), preferred_element_type=F32)


def hot_at(index, count):
    rows = lax.broadcasted_iota(jnp.int32, (count, index.shape[1]), 0)
    return jnp.where(rows == index, 1.0, 0.0).astype(BF)


def spread(values, row, col, rows, cols):
    mask = hot_at(row, rows)
    parts = [two_parts(v) for v in values]
    left = jnp.concatenate([mask * p[k] for k in range(2) for p in parts], axis=0)
    both = nt_dot(left, hot_at(col, cols))
    n = len(values) * rows
    return both[:n] + both[n:]


class Bins:
    def __init__(self, layers, width_x, width_y, span, lines, cols):
        self.layers, self.span, self.lines, self.line = layers, span, lines, cols
        self.binned = lines == span * layers
        self.cols = min(256, width_y)
        self.parts = width_y // self.cols
        self.rows = width_x * self.parts
        self.width_x, self.width_y = width_x, width_y
        self.log_y, self.log_cols = int(math.log2(width_y)), int(math.log2(self.cols))
        self.log_x = int(math.log2(width_x))

    def place(self, ids):
        y = lax.bitwise_and(ids, self.width_y - 1)
        x = lax.bitwise_and(lax.shift_right_arithmetic(ids, self.log_y), self.width_x - 1)
        row = lax.shift_right_arithmetic(y, self.log_cols) * self.width_x + x
        return self.layer(ids) * self.rows + row, lax.bitwise_and(y, self.cols - 1)

    def layer(self, ids):
        return lax.shift_right_arithmetic(ids, self.log_x + self.log_y)

    def strays(self, ids, line, lane):
        live = ids >= 0
        if not self.binned:
            return live
        own = lax.rem(line, self.layers)
        layer = self.layer(ids)
        beside = jnp.where(lane < self.line // 2, own - 1, own + 1)
        return live & (layer != own) & (layer != beside)

    def any_stray(self, ref):
        ids = ref[0].astype(jnp.int32) - 1
        line, lane = (lax.broadcasted_iota(jnp.int32, ids.shape, axis) for axis in range(2))
        mask = self.strays(ids, line, lane)
        return jnp.max(jnp.where(mask, 1.0, 0.0)) > 0.0

    def pieces(self, j):
        half = self.line // 2
        return [
            (pl.ds(o * self.layers + j, 1), slice(h * half, (h + 1) * half))
            for h in range(2)
            for o in range(self.span)
        ]

    def flat(self, ref, c, j):
        return jnp.concatenate([ref[c, line, lanes] for line, lanes in self.pieces(j)], axis=1)

    def group(self, ref, c, g):
        block = ref[c, pl.ds(pl.multiple_of(g * 8, 8), 8), :]
        return jnp.concatenate([block[k : k + 1] for k in range(8)], axis=1)

    def stray_group(self, ref, g):
        ids = self.group(ref, 0, g).astype(jnp.int32) - 1
        lane = lax.broadcasted_iota(jnp.int32, ids.shape, 1)
        shift = int(math.log2(self.line))
        line = g * 8 + lax.shift_right_arithmetic(lane, shift)
        return ids, self.strays(ids, line, lax.bitwise_and(lane, self.line - 1))


def deposit_kernel(bins, recv, out):
    comps = out.shape[0]
    rows, cols, width_x = bins.rows, bins.cols, bins.width_x
    out[...] = jnp.zeros_like(out)

    def add(layer, sums):
        for c in range(comps):
            for part in range(bins.parts):
                lanes = slice(part * cols, (part + 1) * cols)
                first = c * rows + part * width_x
                out[c, layer, :, lanes] += sums[first : first + width_x]

    if bins.binned:

        for j in range(bins.layers):
            flat = [bins.flat(recv, c, j) for c in range(comps + 1)]
            ids = flat[0].astype(jnp.int32) - 1
            place, col = bins.place(ids)
            hot = hot_at(col, cols)
            parts = [two_parts(v) for v in flat[1:]]
            n = ids.shape[1] // 2

            def sums(layer, lanes, place=place, parts=parts, hot=hot):
                mask = hot_at(place[:, lanes] - layer * rows, rows)
                left = [mask * p[k][:, lanes] for k in range(2) for p in parts]
                both = nt_dot(jnp.concatenate(left, axis=0), hot[:, lanes])
                return both[: comps * rows] + both[comps * rows :]

            add(j, sums(j, slice(0, 2 * n)))
            if j > 0:
                add(j - 1, sums(j - 1, slice(0, n)))
            if j < bins.layers - 1:
                add(j + 1, sums(j + 1, slice(n, 2 * n)))

    @pl.when(bins.any_stray(recv))
    def _():
        def line_step(g, carry):
            ids, mask = bins.stray_group(recv, g)
            place, col = bins.place(ids)
            values = [jnp.where(mask, bins.group(recv, 1 + c, g), 0.0) for c in range(comps)]

            def layer_step(layer, inner):
                add(layer, spread(values, place - layer * rows, col, rows, cols))
                return inner

            return lax.fori_loop(0, bins.layers, layer_step, carry)

        lax.fori_loop(0, bins.lines // 8, line_step, 0)

    out[0] = jnp.minimum(out[0], PHI_LIMIT)


def gather_kernel(bins, smooth, ids_ref, fields, out, tables):
    comps = smooth.shape[0]
    rows, cols, width_x = bins.rows, bins.cols, bins.width_x

    def table_step(layer, carry):
        void = 1.0 - smooth[0, layer]
        for c in range(comps):
            value = void if c == 0 else -smooth[c, layer] / void
            fields[c, layer] = value
            high, low = two_parts(value)
            for part in range(bins.parts):
                lanes = slice(part * cols, (part + 1) * cols)
                first = c * rows + part * width_x
                tables[layer, pl.ds(first, width_x)] = high[:, lanes]
                tables[layer, pl.ds(comps * rows + first, width_x)] = low[:, lanes]
        return carry

    lax.fori_loop(0, bins.layers, table_step, 0)

    def found(layer, place, hot):
        wide = jnp.dot(tables[layer], hot, preferred_element_type=F32)
        row = lax.broadcasted_iota(jnp.int32, (rows, place.shape[1]), 0)
        here = row == place
        values = []
        for c in range(comps):
            value = wide[c * rows : (c + 1) * rows] + wide[(comps + c) * rows : (comps + c + 1) * rows]
            values.append(jnp.sum(jnp.where(here, value, 0.0), axis=0, keepdims=True))
        return values

    if bins.binned:
        half = bins.line // 2

        for j in range(bins.layers):
            ids = bins.flat(ids_ref, 0, j).astype(jnp.int32) - 1
            place, col = bins.place(ids)
            hot = hot_at(col, cols)
            n = ids.shape[1] // 2
            own = found(j, place - j * rows, hot)
            low, high = max(j - 1, 0), min(j + 1, bins.layers - 1)
            left = found(low, place[:, :n] - (j - 1) * rows, hot[:, :n])
            right = found(high, place[:, n:] - (j + 1) * rows, hot[:, n:])
            for c in range(comps):
                value = own[c] + jnp.concatenate([left[c], right[c]], axis=1)
                for at, (line, lanes) in enumerate(bins.pieces(j)):
                    out[c, line, lanes] = value[:, at * half : (at + 1) * half]
    else:
        out[...] = jnp.zeros_like(out)

    @pl.when(bins.any_stray(ids_ref))
    def _():
        def line_step(g, carry):
            ids, mask = bins.stray_group(ids_ref, g)
            place, col = bins.place(ids)
            place = jnp.where(mask, place, -1)
            hot = hot_at(col, cols)

            def layer_step(layer, total):
                at = jnp.where(place >= 0, place - layer * rows, -1)
                more = found(layer, at, hot)
                return [t + m for t, m in zip(total, more)]

            zero = [jnp.zeros(ids.shape, F32)] * comps
            total = lax.fori_loop(0, bins.layers, layer_step, zero)
            for c in range(comps):
                n = bins.line
                block = [total[c][:, k * n : (k + 1) * n] for k in range(8)]
                out[c, pl.ds(pl.multiple_of(g * 8, 8), 8), :] += jnp.concatenate(block, axis=0)
            return carry

        lax.fori_loop(0, bins.lines // 8, line_step, 0)


MESH = pl.DeviceIdType.MESH
RIM = SWEEPS // 2
LANES = 128


class Grid:
    def __init__(self):
        self.span, self.depth = lax.axis_index("span"), lax.axis_index("depth")
        self.span_size, self.depth_size = lax.axis_size("span"), lax.axis_size("depth")

    def has(self, dx, dy):
        x, y = self.span + dx, self.depth + dy
        return (x >= 0) & (x < self.span_size) & (y >= 0) & (y < self.depth_size)

    def peer(self, dx, dy):
        return (self.span + dx, self.depth + dy)

    def signal(self, barrier, dx, dy):
        @pl.when(self.has(dx, dy))
        def _():
            pl.semaphore_signal(barrier, inc=1, device_id=self.peer(dx, dy), device_id_type=MESH)

    def around(self, steps):
        return sum(self.has(dx, dy).astype(jnp.int32) for dx, dy in steps)


X_STEPS = ((-1, 0), (1, 0))
Y_STEPS = ((0, -1), (0, 1))


class Halo:
    def __init__(self, grid, rows_out, rows_in, edge, columns, send_sem, recv_sem):
        self.grid = grid
        self.rows_out, self.rows_in, self.edge, self.columns = rows_out, rows_in, edge, columns
        self.send_sem, self.recv_sem = send_sem, recv_sem

    def _copy(self, src, dst, at, step):
        return pltpu.make_async_remote_copy(
            src_ref=src,
            dst_ref=dst,
            send_sem=self.send_sem(at),
            recv_sem=self.recv_sem(at),
            device_id=self.grid.peer(*step),
            device_id_type=MESH,
        )

    def rows(self, side):
        return self._copy(self.rows_out(side), self.rows_in(1 - side), side, X_STEPS[side])

    def cols(self, part, side):
        at = 2 + 2 * part + side
        return self._copy(self.edge(part, side), self.columns(part, 1 - side), at, Y_STEPS[side])

    def _when(self, step, action):
        @pl.when(self.grid.has(*step))
        def _():
            action()

    def start(self):
        for side in range(2):
            self._when(X_STEPS[side], lambda: self.rows(side).start())
        for side in range(2):
            self._when(Y_STEPS[side], lambda: self.cols(0, side).start())

    def forward(self):
        for side in range(2):
            self._when(X_STEPS[1 - side], lambda: self.rows(side).wait_recv())
        for part in (1, 2):
            for side in range(2):
                self._when(Y_STEPS[side], lambda: self.cols(part, side).start())

    def arrive(self):
        for part in range(3):
            for side in range(2):
                self._when(Y_STEPS[1 - side], lambda: self.cols(part, side).wait_recv())

    def sent(self):
        for side in range(2):
            self._when(X_STEPS[side], lambda: self.rows(side).wait_send())
        for part in range(3):
            for side in range(2):
                self._when(Y_STEPS[side], lambda: self.cols(part, side).wait_send())


HALO_COPIES = 8


def collect_kernel(
    cap, block, wide, layers, shift, count, slab, cell, volume, drag, solid, prior,
    recv, slots, rows_in, cols_in, packed, rows_out, cols_out,
    halo_send, halo_recv, send_sem, recv_sem, own_sem,
):
    grid = Grid()
    span_size = grid.span_size
    values, _, per, cols = recv.shape
    lines = span_size * per
    part_rows = slab.shape[1]
    width_x, width_y = solid.shape[1:]
    comps = 1 + prior.shape[0]
    total_x = width_x + 2 * RIM

    barrier = pltpu.get_barrier_semaphore()
    for k in range(1, span_size):
        to = lax.rem(grid.span + k, span_size)
        pl.semaphore_signal(barrier, inc=1, device_id=(to, grid.depth), device_id_type=MESH)
    for dx, dy in Y_STEPS:
        grid.signal(barrier, dx, dy)

    for c in range(comps):
        field = solid if c == 0 else prior.at[c - 1]
        for x in range(width_x):
            line = field[:, x, :]
            if x < RIM:
                rows_out[c, 0, x] = line
            if x >= width_x - RIM:
                rows_out[c, 1, x - width_x + RIM] = line
            cols_out[c, 0, x] = line[:, :LANES]
            cols_out[c, 1, x] = line[:, width_y - LANES :]
    for side in range(2):

        @pl.when(jnp.logical_not(grid.has(*X_STEPS[side])))
        def _(side=side):
            rows_in[:, side] = jnp.zeros((comps, RIM, layers, width_y), F32)

        @pl.when(jnp.logical_not(grid.has(*Y_STEPS[side])))
        def _(side=side):
            cols_in[:, side] = jnp.zeros((comps, total_x, layers, LANES), F32)

    def edge(part, side):
        if part == 0:
            return cols_out.at[:, side]
        lanes = pl.ds(0 if side == 0 else width_y - LANES, LANES)
        return rows_in.at[:, part - 1, :, :, lanes]

    def columns(part, side):
        first, number = ((RIM, width_x), (0, RIM), (RIM + width_x, RIM))[part]
        return cols_in.at[:, side, pl.ds(first, number)]

    halo = Halo(
        grid, lambda side: rows_out.at[:, side], lambda side: rows_in.at[:, side], edge, columns,
        lambda at: halo_send.at[at], lambda at: halo_recv.at[at],
    )
    pl.semaphore_wait(barrier, span_size - 1 + grid.around(Y_STEPS))
    halo.start()

    keys = layers * span_size
    before_lane = lax.broadcasted_iota(jnp.int32, (block, block), 0)
    this_lane = lax.broadcasted_iota(jnp.int32, (block, block), 1)
    tri = jnp.where(before_lane < this_lane, 1.0, 0.0).astype(BF)
    live_count = count[0, 0]
    many = wide // block

    def lanes_at(first, size):
        return pl.ds(pl.multiple_of(first, size), size)

    def member_of(first):
        lanes = lanes_at(first, block)
        live = first + lax.broadcasted_iota(jnp.int32, (1, block), 1) < live_count
        layer = lax.shift_right_arithmetic(cell[:, lanes], shift)
        key = jnp.where(live, layer * span_size + slab[:, lanes], -1)
        member = jnp.where(lax.broadcasted_iota(jnp.int32, (keys, block), 0) == key, 1.0, 0.0)
        return member, live

    fold = min(block, LANES)

    def tally(b, total):
        for m in range(many):
            member = member_of(b * wide + m * block)[0]
            for k in range(block // fold):
                total = total + member[:, k * fold : (k + 1) * fold]
        return total

    total = lax.fori_loop(0, part_rows // wide, tally, jnp.zeros((keys, fold), F32))
    total = jnp.sum(total, axis=1, keepdims=True)
    counts = [total[k * span_size : (k + 1) * span_size] for k in range(layers)]
    rest = [None] * layers
    left = jnp.zeros((span_size, 1), F32)
    for k in reversed(range(layers)):
        left = left + counts[k]
        rest[k] = left
    base = lax.broadcasted_iota(jnp.int32, (span_size, 1), 0).astype(F32) * cap
    end = jnp.zeros((span_size, 1), F32)
    starts = []
    for k in range(layers):
        start = jnp.minimum(jnp.maximum(end, float(cap // layers * k)), cap - rest[k])
        starts.append(start + base)
        end = start + counts[k]

    def rank(b, offset):
        for m in range(many):
            first = b * wide + m * block
            member, live = member_of(first)
            before = jnp.dot(member.astype(BF), tri, preferred_element_type=F32)
            place = jnp.sum(member * (before + offset), axis=0, keepdims=True).astype(jnp.int32)
            slots[:, lanes_at(first, block)] = jnp.where(live, place, -1)
            offset = offset + jnp.sum(member, axis=1, keepdims=True)
        return offset

    lax.fori_loop(0, part_rows // wide, rank, jnp.concatenate(starts, axis=0))

    groups = ((0, 2), (2, values - 2))
    copies = []
    for at, (first_value, number) in enumerate(groups):
        mine = pl.ds(first_value, number)

        def place_values(b, carry, first_value=first_value, number=number, mine=mine):
            lanes = lanes_at(b * wide, wide)
            slot = slots[:, lanes]
            row = lax.shift_right_arithmetic(slot, int(math.log2(cols)))
            col = lax.bitwise_and(slot, cols - 1)
            taken = []
            for v in range(first_value, first_value + number):
                if v == 0:
                    taken.append((cell[:, lanes] + 1).astype(F32))
                else:
                    taken.append(volume[:, lanes] if v == 1 else drag[v - 2, :, lanes])
            sums = spread(taken, row, col, lines, cols).reshape(number, span_size, per, cols)
            packed[mine] += sums
            return carry

        packed[mine] = jnp.zeros((number, span_size, per, cols), F32)
        lax.fori_loop(0, part_rows // wide, place_values, 0)
        own = pltpu.make_async_copy(
            packed.at[mine, grid.span], recv.at[mine, grid.span], own_sem.at[at]
        )
        own.start()
        copies.append(own)
        for k in range(1, span_size):
            to = lax.rem(grid.span + k, span_size)
            copies.append(
                pltpu.make_async_remote_copy(
                    src_ref=packed.at[mine, to],
                    dst_ref=recv.at[mine, grid.span],
                    send_sem=send_sem.at[at, k],
                    recv_sem=recv_sem.at[at, k],
                    device_id=(to, grid.depth),
                    device_id_type=MESH,
                )
            )
            copies[-1].start()
        if at == 0:
            halo.forward()
    halo.arrive()
    for copy in copies:
        copy.wait()
    halo.sent()


def sweeps_kernel(
    solid, prior, prior_rows, prior_cols, target, out,
    source, first, second, middle, source_cols, middle_cols, send_sem, recv_sem,
):
    grid = Grid()
    comps, layers, width_x, width_y = target.shape
    total_x = width_x + 2 * RIM
    own = pl.ds(0, width_y)
    rest = pl.ds(width_y, LANES)
    own_rows = pl.ds(RIM, width_x)

    barrier = pltpu.get_barrier_semaphore()
    for dx, dy in X_STEPS + Y_STEPS:
        grid.signal(barrier, dx, dy)

    def halo_of(c, phase):
        buffer, cols_in = (source, source_cols) if phase == 0 else (middle, middle_cols)
        width = RIM - 1 if phase == 0 else RIM

        def rows_out(side):
            return buffer.at[c, pl.ds(RIM if side == 0 else RIM + width_x - width, width), :, own]

        def rows_in(side):
            return buffer.at[c, pl.ds(RIM - width if side == 0 else RIM + width_x, width), :, own]

        def rows_of(part):
            return pl.ds(*((RIM, width_x), (RIM - width, width), (RIM + width_x, width))[part])

        def edge(part, side):
            lanes = pl.ds(0 if side == 0 else width_y - LANES, LANES)
            return buffer.at[c, rows_of(part), :, lanes]

        def columns(part, side):
            return cols_in.at[c, side, rows_of(part)]

        return Halo(
            grid, rows_out, rows_in, edge, columns,
            lambda at: send_sem.at[c, phase, at], lambda at: recv_sem.at[c, phase, at],
        )

    halos = [[halo_of(c, phase) for phase in range(2)] for c in range(comps)]
    lane = lax.broadcasted_iota(jnp.int32, (1, layers, LANES), 2)

    def fill_cols(buffer, c, cols_in):
        buffer[c, :, :, rest] = jnp.where(lane < LANES // 2, cols_in[c, 1], cols_in[c, 0])

    for c in range(comps):
        for x in range(width_x):
            source[c, RIM + x, :, own] = target[c, :, x, :]
        if c == 0:
            pl.semaphore_wait(barrier, grid.around(X_STEPS + Y_STEPS))
        halos[c][0].start()
    for side, at in ((0, 0), (1, RIM + width_x)):

        @pl.when(jnp.logical_not(grid.has(*X_STEPS[side])))
        def _(at=at):
            for buffer in (source, middle):
                zeros = jnp.zeros((comps, RIM, layers, width_y), F32)
                buffer[:, pl.ds(at, RIM), :, own] = zeros

        @pl.when(jnp.logical_not(grid.has(*Y_STEPS[side])))
        def _(side=side):
            for buffer in (source_cols, middle_cols):
                buffer[:, side] = jnp.zeros((comps, total_x, layers, LANES), F32)

    for c in range(comps):
        field = solid if c == 0 else prior.at[c - 1]
        for x in range(width_x):
            first[c, RIM + x, :, own] = field[:, x, :]
        first[c, pl.ds(0, RIM), :, own] = prior_rows[c, 0]
        first[c, pl.ds(RIM + width_x, RIM), :, own] = prior_rows[c, 1]
        fill_cols(first, c, prior_cols)

    lanes = lax.broadcasted_iota(jnp.int32, (layers, width_y + LANES), 1)
    known = lanes < width_y
    known = known | ((lanes < width_y + LANES // 2) & (grid.depth < grid.depth_size - 1))
    known = known | ((lanes >= width_y + LANES // 2) & (grid.depth > 0))
    scale = jnp.where(known, 1.0 / (1.0 + 4.0 * NU_WEIGHT), 0.0)

    def relax(c, x, before, here, after):
        beside = before + after
        beside = beside + pltpu.roll(here, 1, 1) + pltpu.roll(here, width_y + LANES - 1, 1)
        return (source[c, x] + NU_WEIGHT * beside) * scale

    def sweep(c, old, new, gone):
        low, high = gone, total_x - gone
        step = max(k for k in range(1, 9) if (high - low) % k == 0)

        def rows(g, carry):
            before, here = carry
            for k in range(step):
                x = low + g * step + k
                after = old[c, x + 1]
                new[c, x] = relax(c, x, before, here, after)
                before, here = here, after
            return before, here

        lax.fori_loop(0, (high - low) // step, rows, (old[c, low - 1], old[c, low]))
        for side, x in ((0, RIM - 1), (1, RIM + width_x)):
            if low <= x < high:

                @pl.when(jnp.logical_not(grid.has(*X_STEPS[side])))
                def _(x=x):
                    new[c, x] = jnp.zeros((layers, width_y + LANES), F32)

    def first_half(c):
        halos[c][0].arrive()
        fill_cols(source, c, source_cols)
        sweep(c, first, second, 1)
        sweep(c, second, first, 2)
        sweep(c, first, middle, 3)
        halos[c][1].start()

    def second_half(c):
        halos[c][1].arrive()
        fill_cols(middle, c, middle_cols)
        sweep(c, middle, first, 1)
        sweep(c, first, second, 2)
        before, here = second[c, RIM - 1], second[c, RIM]
        for x in range(width_x):
            after = second[c, RIM + x + 1]
            out[c, :, x, :] = relax(c, RIM + x, before, here, after)[:, :width_y]
            before, here = here, after

    halos[0][0].forward()
    for c in range(comps):
        if c + 1 < comps:
            halos[c + 1][0].forward()
        first_half(c)
    halos[0][1].forward()
    for c in range(comps):
        if c + 1 < comps:
            halos[c + 1][1].forward()
        second_half(c)
    for c in range(comps):
        for phase in range(2):
            halos[c][phase].sent()


def feedback_kernel(wide, values, slots, out, table, hots, send_sem, recv_sem, own_sem):
    grid = Grid()
    comps, span_size, per, cols = values.shape
    lines = span_size * per
    part_rows = slots.shape[1]
    barrier = pltpu.get_barrier_semaphore()
    for k in range(1, span_size):
        to = lax.rem(grid.span + k, span_size)
        pl.semaphore_signal(barrier, inc=1, device_id=(to, grid.depth), device_id_type=MESH)
    pl.semaphore_wait(barrier, span_size - 1)
    groups = (pl.ds(0, comps // 2), pl.ds(comps // 2, comps - comps // 2))
    copies = []
    for at, mine in enumerate(groups):
        own = pltpu.make_async_copy(
            values.at[mine, grid.span], table.at[mine, grid.span], own_sem.at[at]
        )
        own.start()
        copies.append([own])
        for k in range(1, span_size):
            to = lax.rem(grid.span + k, span_size)
            copies[at].append(
                pltpu.make_async_remote_copy(
                    src_ref=values.at[mine, to],
                    dst_ref=table.at[mine, grid.span],
                    send_sem=send_sem.at[at, k],
                    recv_sem=recv_sem.at[at, k],
                    device_id=(to, grid.depth),
                    device_id_type=MESH,
                )
            )
            copies[at][-1].start()

    def lanes_at(b):
        return pl.ds(pl.multiple_of(b * wide, wide), wide)

    def hot_step(b, carry):
        lanes = lanes_at(b)
        hots[:, lanes] = hot_at(lax.bitwise_and(slots[:, lanes], cols - 1), cols)
        return carry

    lax.fori_loop(0, part_rows // wide, hot_step, 0)
    for at, mine in enumerate(groups):
        for copy in copies[at]:
            copy.wait()
        number = mine.size
        high, low = two_parts(table[mine].reshape(number * lines, cols))
        both = jnp.concatenate([high, low], axis=0)

        def pick_step(b, carry, mine=mine, number=number, both=both):
            lanes = lanes_at(b)
            row = lax.shift_right_arithmetic(slots[:, lanes], int(math.log2(cols)))
            wanted = lax.broadcasted_iota(jnp.int32, (lines, wide), 0) == row
            found = jnp.dot(both, hots[:, lanes], preferred_element_type=F32)
            for c in range(number):
                value = found[c * lines : (c + 1) * lines]
                value = value + found[(number + c) * lines : (number + c + 1) * lines]
                value = jnp.sum(jnp.where(wanted, value, 0.0), axis=0, keepdims=True)
                out[mine.start + c, :, lanes] = value
            return carry

        lax.fori_loop(0, part_rows // wide, pick_step, 0)


VMEM = pl.BlockSpec(memory_space=pltpu.VMEM)
SMEM = pl.BlockSpec(memory_space=pltpu.SMEM)
LIMIT = pltpu.CompilerParams(vmem_limit_bytes=48 * 1024 * 1024)


def far(number):
    return pltpu.CompilerParams(
        vmem_limit_bytes=48 * 1024 * 1024, collective_id=number, has_side_effects=True
    )


def on_device(part_slab, part_cell, part_volume, part_drag, part_count, prior_solid, prior_drag):
    span_size = lax.axis_size("span")
    part_rows = part_cell.shape[1]
    cap = 2 * part_rows // span_size
    layers, width_x, width_y = prior_solid.shape
    cols = min(256, cap)
    lines = span_size * cap // cols
    per = lines // span_size
    block = math.gcd(part_rows, 512)
    wide = math.gcd(part_rows, 2048)
    total_x = width_x + 2 * RIM
    dma = pltpu.SemaphoreType.DMA
    recv, slots, prior_rows, prior_cols = pl.pallas_call(
        functools.partial(
            collect_kernel, cap, block, wide, layers, int(math.log2(width_x * width_y))
        ),
        out_shape=(
            jax.ShapeDtypeStruct((5, span_size, per, cols), F32),
            jax.ShapeDtypeStruct((1, part_rows), jnp.int32),
            jax.ShapeDtypeStruct((4, 2, RIM, layers, width_y), F32),
            jax.ShapeDtypeStruct((4, 2, total_x, layers, LANES), F32),
        ),
        in_specs=[SMEM] + [VMEM] * 6,
        out_specs=(VMEM,) * 4,
        scratch_shapes=[
            pltpu.VMEM((5, span_size, per, cols), F32),
            pltpu.VMEM((4, 2, RIM, layers, width_y), F32),
            pltpu.VMEM((4, 2, width_x, layers, LANES), F32),
            dma((HALO_COPIES,)),
            dma((HALO_COPIES,)),
            dma((2, span_size)),
            dma((2, span_size)),
            dma((2,)),
        ],
        compiler_params=far(1),
        name="collect",
    )(
        part_count, part_slab.reshape(1, part_rows), part_cell, part_volume, part_drag,
        prior_solid, prior_drag,
    )
    recv = recv.reshape(5, lines, cols)
    bins = Bins(layers, width_x, width_y, span_size, lines, cols)
    target = pl.pallas_call(
        functools.partial(deposit_kernel, bins),
        out_shape=jax.ShapeDtypeStruct((4, layers, width_x, width_y), F32),
        in_specs=[VMEM],
        out_specs=VMEM,
        compiler_params=LIMIT,
        name="deposit",
    )(recv)
    whole = pltpu.VMEM((4, total_x, layers, width_y + LANES), F32)
    columns = pltpu.VMEM((4, 2, total_x, layers, LANES), F32)
    smooth = pl.pallas_call(
        sweeps_kernel,
        out_shape=jax.ShapeDtypeStruct(target.shape, F32),
        in_specs=[VMEM] * 5,
        out_specs=VMEM,
        scratch_shapes=[whole] * 4 + [columns] * 2 + [dma((4, 2, HALO_COPIES))] * 2,
        compiler_params=far(0),
        name="sweeps",
    )(prior_solid, prior_drag, prior_rows, prior_cols, target)
    fields, values = pl.pallas_call(
        functools.partial(gather_kernel, bins),
        out_shape=(
            jax.ShapeDtypeStruct((4, layers, width_x, width_y), F32),
            jax.ShapeDtypeStruct((4, lines, cols), F32),
        ),
        in_specs=[VMEM] * 2,
        out_specs=(VMEM, VMEM),
        scratch_shapes=[pltpu.VMEM((layers, 8 * bins.rows, bins.cols), BF)],
        compiler_params=LIMIT,
        name="gather",
    )(smooth, recv)
    feedback = pl.pallas_call(
        functools.partial(feedback_kernel, wide),
        out_shape=jax.ShapeDtypeStruct((4, 1, part_rows), F32),
        in_specs=[VMEM] * 2,
        out_specs=VMEM,
        scratch_shapes=[
            pltpu.VMEM((4, span_size, per, cols), F32),
            pltpu.VMEM((cols, part_rows), BF),
            dma((2, span_size)),
            dma((2, span_size)),
            dma((2,)),
        ],
        compiler_params=far(2),
        name="feedback",
    )(values.reshape(4, span_size, per, cols), slots)
    return (fields, feedback)


def solution(mesh):
    in_specs = (
        P("depth", "span", None),
        P("depth", "span"),
        P("depth", "span"),
        P(None, "depth", "span"),
        P("depth", "span"),
        P(None, "span", "depth"),
        P(None, None, "span", "depth"),
    )
    out_specs = (P(None, None, "span", "depth"), P(None, "depth", "span"))
    return jax.shard_map(
        on_device, mesh=mesh, in_specs=in_specs, out_specs=out_specs, check_vma=False
    )
```

```python
import functools
import math

import jax
import jax.numpy as jnp
from jax import lax
from jax.experimental import pallas as pl
from jax.experimental.pallas import tpu as pltpu
from jax.sharding import PartitionSpec as P

SWEEPS = 6
NU_WEIGHT = 1.0
PHI_LIMIT = 0.6
BF = jnp.bfloat16
F32 = jnp.float32


def two_parts(value):
    high = value.astype(BF)
    return high, (value - high.astype(F32)).astype(BF)


def nt_dot(left, right):
    return lax.dot_general(left, right, (((1,), (1,)), ((), ())), preferred_element_type=F32)


def hot_at(index, count):
    rows = lax.broadcasted_iota(jnp.int32, (count, index.shape[1]), 0)
    return jnp.where(rows == index, 1.0, 0.0).astype(BF)


def spread(values, row, col, rows, cols):
    mask = hot_at(row, rows)
    parts = [two_parts(v) for v in values]
    left = jnp.concatenate([mask * p[k] for k in range(2) for p in parts], axis=0)
    both = nt_dot(left, hot_at(col, cols))
    n = len(values) * rows
    return both[:n] + both[n:]


class Bins:
    def __init__(self, layers, width_x, width_y, span, lines, cols):
        self.layers, self.span, self.lines, self.line = layers, span, lines, cols
        self.binned = lines == span * layers
        self.cols = min(256, width_y)
        self.parts = width_y // self.cols
        self.rows = width_x * self.parts
        self.width_x, self.width_y = width_x, width_y
        self.log_y, self.log_cols = int(math.log2(width_y)), int(math.log2(self.cols))
        self.log_x = int(math.log2(width_x))

    def place(self, ids):
        y = lax.bitwise_and(ids, self.width_y - 1)
        x = lax.bitwise_and(lax.shift_right_arithmetic(ids, self.log_y), self.width_x - 1)
        row = lax.shift_right_arithmetic(y, self.log_cols) * self.width_x + x
        return self.layer(ids) * self.rows + row, lax.bitwise_and(y, self.cols - 1)

    def layer(self, ids):
        return lax.shift_right_arithmetic(ids, self.log_x + self.log_y)

    def strays(self, ids, line, lane):
        live = ids >= 0
        if not self.binned:
            return live
        own = lax.rem(line, self.layers)
        layer = self.layer(ids)
        beside = jnp.where(lane < self.line // 2, own - 1, own + 1)
        return live & (layer != own) & (layer != beside)

    def any_stray(self, ref):
        ids = ref[0].astype(jnp.int32) - 1
        line, lane = (lax.broadcasted_iota(jnp.int32, ids.shape, axis) for axis in range(2))
        mask = self.strays(ids, line, lane)
        return jnp.max(jnp.where(mask, 1.0, 0.0)) > 0.0

    def pieces(self, j):
        half = self.line // 2
        return [
            (pl.ds(o * self.layers + j, 1), slice(h * half, (h + 1) * half))
            for h in range(2)
            for o in range(self.span)
        ]

    def flat(self, ref, c, j):
        return jnp.concatenate([ref[c, line, lanes] for line, lanes in self.pieces(j)], axis=1)

    def group(self, ref, c, g):
        block = ref[c, pl.ds(pl.multiple_of(g * 8, 8), 8), :]
        return jnp.concatenate([block[k : k + 1] for k in range(8)], axis=1)

    def stray_group(self, ref, g):
        ids = self.group(ref, 0, g).astype(jnp.int32) - 1
        lane = lax.broadcasted_iota(jnp.int32, ids.shape, 1)
        shift = int(math.log2(self.line))
        line = g * 8 + lax.shift_right_arithmetic(lane, shift)
        return ids, self.strays(ids, line, lax.bitwise_and(lane, self.line - 1))


def deposit_kernel(bins, recv, out):
    comps = out.shape[0]
    rows, cols, width_x = bins.rows, bins.cols, bins.width_x
    out[...] = jnp.zeros_like(out)

    def add(layer, sums):
        for c in range(comps):
            for part in range(bins.parts):
                lanes = slice(part * cols, (part + 1) * cols)
                first = c * rows + part * width_x
                out[c, layer, :, lanes] += sums[first : first + width_x]

    if bins.binned:

        for j in range(bins.layers):
            flat = [bins.flat(recv, c, j) for c in range(comps + 1)]
            ids = flat[0].astype(jnp.int32) - 1
            place, col = bins.place(ids)
            hot = hot_at(col, cols)
            parts = [two_parts(v) for v in flat[1:]]
            n = ids.shape[1] // 2

            def sums(layer, lanes, place=place, parts=parts, hot=hot):
                mask = hot_at(place[:, lanes] - layer * rows, rows)
                left = [mask * p[k][:, lanes] for k in range(2) for p in parts]
                both = nt_dot(jnp.concatenate(left, axis=0), hot[:, lanes])
                return both[: comps * rows] + both[comps * rows :]

            add(j, sums(j, slice(0, 2 * n)))
            if j > 0:
                add(j - 1, sums(j - 1, slice(0, n)))
            if j < bins.layers - 1:
                add(j + 1, sums(j + 1, slice(n, 2 * n)))

    @pl.when(bins.any_stray(recv))
    def _():
        def line_step(g, carry):
            ids, mask = bins.stray_group(recv, g)
            place, col = bins.place(ids)
            values = [jnp.where(mask, bins.group(recv, 1 + c, g), 0.0) for c in range(comps)]

            def layer_step(layer, inner):
                add(layer, spread(values, place - layer * rows, col, rows, cols))
                return inner

            return lax.fori_loop(0, bins.layers, layer_step, carry)

        lax.fori_loop(0, bins.lines // 8, line_step, 0)

    out[0] = jnp.minimum(out[0], PHI_LIMIT)


def gather_kernel(bins, smooth, ids_ref, fields, out, tables):
    comps = smooth.shape[0]
    rows, cols, width_x = bins.rows, bins.cols, bins.width_x

    def table_step(layer, carry):
        void = 1.0 - smooth[0, layer]
        for c in range(comps):
            value = void if c == 0 else -smooth[c, layer] / void
            fields[c, layer] = value
            high, low = two_parts(value)
            for part in range(bins.parts):
                lanes = slice(part * cols, (part + 1) * cols)
                first = c * rows + part * width_x
                tables[layer, pl.ds(first, width_x)] = high[:, lanes]
                tables[layer, pl.ds(comps * rows + first, width_x)] = low[:, lanes]
        return carry

    lax.fori_loop(0, bins.layers, table_step, 0)

    def found(layer, place, hot):
        wide = jnp.dot(tables[layer], hot, preferred_element_type=F32)
        row = lax.broadcasted_iota(jnp.int32, (rows, place.shape[1]), 0)
        here = row == place
        values = []
        for c in range(comps):
            value = wide[c * rows : (c + 1) * rows] + wide[(comps + c) * rows : (comps + c + 1) * rows]
            values.append(jnp.sum(jnp.where(here, value, 0.0), axis=0, keepdims=True))
        return values

    if bins.binned:
        half = bins.line // 2

        for j in range(bins.layers):
            ids = bins.flat(ids_ref, 0, j).astype(jnp.int32) - 1
            place, col = bins.place(ids)
            hot = hot_at(col, cols)
            n = ids.shape[1] // 2
            own = found(j, place - j * rows, hot)
            low, high = max(j - 1, 0), min(j + 1, bins.layers - 1)
            left = found(low, place[:, :n] - (j - 1) * rows, hot[:, :n])
            right = found(high, place[:, n:] - (j + 1) * rows, hot[:, n:])
            for c in range(comps):
                value = own[c] + jnp.concatenate([left[c], right[c]], axis=1)
                for at, (line, lanes) in enumerate(bins.pieces(j)):
                    out[c, line, lanes] = value[:, at * half : (at + 1) * half]
    else:
        out[...] = jnp.zeros_like(out)

    @pl.when(bins.any_stray(ids_ref))
    def _():
        def line_step(g, carry):
            ids, mask = bins.stray_group(ids_ref, g)
            place, col = bins.place(ids)
            place = jnp.where(mask, place, -1)
            hot = hot_at(col, cols)

            def layer_step(layer, total):
                at = jnp.where(place >= 0, place - layer * rows, -1)
                more = found(layer, at, hot)
                return [t + m for t, m in zip(total, more)]

            zero = [jnp.zeros(ids.shape, F32)] * comps
            total = lax.fori_loop(0, bins.layers, layer_step, zero)
            for c in range(comps):
                n = bins.line
                block = [total[c][:, k * n : (k + 1) * n] for k in range(8)]
                out[c, pl.ds(pl.multiple_of(g * 8, 8), 8), :] += jnp.concatenate(block, axis=0)
            return carry

        lax.fori_loop(0, bins.lines // 8, line_step, 0)


MESH = pl.DeviceIdType.MESH
RIM = SWEEPS // 2
LANES = 128


class Grid:
    def __init__(self):
        self.span, self.depth = lax.axis_index("span"), lax.axis_index("depth")
        self.span_size, self.depth_size = lax.axis_size("span"), lax.axis_size("depth")

    def has(self, dx, dy):
        x, y = self.span + dx, self.depth + dy
        return (x >= 0) & (x < self.span_size) & (y >= 0) & (y < self.depth_size)

    def peer(self, dx, dy):
        return (self.span + dx, self.depth + dy)

    def signal(self, barrier, dx, dy):
        @pl.when(self.has(dx, dy))
        def _():
            pl.semaphore_signal(barrier, inc=1, device_id=self.peer(dx, dy), device_id_type=MESH)

    def around(self, steps):
        return sum(self.has(dx, dy).astype(jnp.int32) for dx, dy in steps)


X_STEPS = ((-1, 0), (1, 0))
Y_STEPS = ((0, -1), (0, 1))


class Halo:
    def __init__(self, grid, rows_out, rows_in, edge, columns, send_sem, recv_sem):
        self.grid = grid
        self.rows_out, self.rows_in, self.edge, self.columns = rows_out, rows_in, edge, columns
        self.send_sem, self.recv_sem = send_sem, recv_sem

    def _copy(self, src, dst, at, step):
        return pltpu.make_async_remote_copy(
            src_ref=src,
            dst_ref=dst,
            send_sem=self.send_sem(at),
            recv_sem=self.recv_sem(at),
            device_id=self.grid.peer(*step),
            device_id_type=MESH,
        )

    def rows(self, side):
        return self._copy(self.rows_out(side), self.rows_in(1 - side), side, X_STEPS[side])

    def cols(self, part, side):
        at = 2 + 2 * part + side
        return self._copy(self.edge(part, side), self.columns(part, 1 - side), at, Y_STEPS[side])

    def _when(self, step, action):
        @pl.when(self.grid.has(*step))
        def _():
            action()

    def start(self):
        for side in range(2):
            self._when(X_STEPS[side], lambda: self.rows(side).start())
        for side in range(2):
            self._when(Y_STEPS[side], lambda: self.cols(0, side).start())

    def forward(self):
        for side in range(2):
            self._when(X_STEPS[1 - side], lambda: self.rows(side).wait_recv())
        for part in (1, 2):
            for side in range(2):
                self._when(Y_STEPS[side], lambda: self.cols(part, side).start())

    def arrive(self):
        for part in range(3):
            for side in range(2):
                self._when(Y_STEPS[1 - side], lambda: self.cols(part, side).wait_recv())

    def sent(self):
        for side in range(2):
            self._when(X_STEPS[side], lambda: self.rows(side).wait_send())
        for part in range(3):
            for side in range(2):
                self._when(Y_STEPS[side], lambda: self.cols(part, side).wait_send())


HALO_COPIES = 8


def collect_kernel(
    cap, block, wide, layers, shift, count, slab_far, cell_far, volume_far, drag_far, solid_far,
    prior_far, recv, slots, rows_in, cols_in, packed, rows_out, cols_out,
    slab, cell, volume, drag, solid, prior, halo_send, halo_recv, send_sem, recv_sem, own_sem,
    near_sem,
):
    pairs = (
        (slab_far, slab), (cell_far, cell), (solid_far, solid), (prior_far, prior),
        (volume_far, volume), (drag_far, drag),
    )
    near = [pltpu.make_async_copy(a, b, near_sem.at[k]) for k, (a, b) in enumerate(pairs)]
    for copy in near:
        copy.start()
    grid = Grid()
    span_size = grid.span_size
    values, _, per, cols = recv.shape
    lines = span_size * per
    part_rows = slab.shape[1]
    width_x, width_y = solid.shape[1:]
    comps = 1 + prior.shape[0]
    total_x = width_x + 2 * RIM

    barrier = pltpu.get_barrier_semaphore()
    for k in range(1, span_size):
        to = lax.rem(grid.span + k, span_size)
        pl.semaphore_signal(barrier, inc=1, device_id=(to, grid.depth), device_id_type=MESH)
    for dx, dy in Y_STEPS:
        grid.signal(barrier, dx, dy)

    keys = layers * span_size
    live_count = count[0, 0]
    many = wide // block

    def lanes_at(first, size):
        return pl.ds(pl.multiple_of(first, size), size)

    def member_of(first):
        lanes = lanes_at(first, block)
        live = first + lax.broadcasted_iota(jnp.int32, (1, block), 1) < live_count
        layer = lax.shift_right_arithmetic(cell[:, lanes], shift)
        key = jnp.where(live, layer * span_size + slab[:, lanes], -1)
        member = jnp.where(lax.broadcasted_iota(jnp.int32, (keys, block), 0) == key, 1.0, 0.0)
        return member, live

    fold = min(block, LANES)

    def tally(b, total):
        for m in range(many):
            member = member_of(b * wide + m * block)[0]
            for k in range(block // fold):
                total = total + member[:, k * fold : (k + 1) * fold]
        return total

    near[0].wait()
    near[1].wait()
    total = lax.fori_loop(0, part_rows // wide, tally, jnp.zeros((keys, fold), F32))
    near[2].wait()
    near[3].wait()
    for c in range(comps):
        field = solid if c == 0 else prior.at[c - 1]
        for x in range(width_x):
            line = field[:, x, :]
            if x < RIM:
                rows_out[c, 0, x] = line
            if x >= width_x - RIM:
                rows_out[c, 1, x - width_x + RIM] = line
            cols_out[c, 0, x] = line[:, :LANES]
            cols_out[c, 1, x] = line[:, width_y - LANES :]
    for side in range(2):

        @pl.when(jnp.logical_not(grid.has(*X_STEPS[side])))
        def _(side=side):
            rows_in[:, side] = jnp.zeros((comps, RIM, layers, width_y), F32)

        @pl.when(jnp.logical_not(grid.has(*Y_STEPS[side])))
        def _(side=side):
            cols_in[:, side] = jnp.zeros((comps, total_x, layers, LANES), F32)

    def edge(part, side):
        if part == 0:
            return cols_out.at[:, side]
        lanes = pl.ds(0 if side == 0 else width_y - LANES, LANES)
        return rows_in.at[:, part - 1, :, :, lanes]

    def columns(part, side):
        first, number = ((RIM, width_x), (0, RIM), (RIM + width_x, RIM))[part]
        return cols_in.at[:, side, pl.ds(first, number)]

    halo = Halo(
        grid, lambda side: rows_out.at[:, side], lambda side: rows_in.at[:, side], edge, columns,
        lambda at: halo_send.at[at], lambda at: halo_recv.at[at],
    )
    pl.semaphore_wait(barrier, span_size - 1 + grid.around(Y_STEPS))
    halo.start()

    before_lane = lax.broadcasted_iota(jnp.int32, (block, block), 0)
    this_lane = lax.broadcasted_iota(jnp.int32, (block, block), 1)
    tri = jnp.where(before_lane < this_lane, 1.0, 0.0).astype(BF)
    total = jnp.sum(total, axis=1, keepdims=True)
    counts = [total[k * span_size : (k + 1) * span_size] for k in range(layers)]
    rest = [None] * layers
    left = jnp.zeros((span_size, 1), F32)
    for k in reversed(range(layers)):
        left = left + counts[k]
        rest[k] = left
    base = lax.broadcasted_iota(jnp.int32, (span_size, 1), 0).astype(F32) * cap
    end = jnp.zeros((span_size, 1), F32)
    starts = []
    for k in range(layers):
        start = jnp.minimum(jnp.maximum(end, float(cap // layers * k)), cap - rest[k])
        starts.append(start + base)
        end = start + counts[k]

    def rank(b, offset):
        for m in range(many):
            first = b * wide + m * block
            member, live = member_of(first)
            before = jnp.dot(member.astype(BF), tri, preferred_element_type=F32)
            place = jnp.sum(member * (before + offset), axis=0, keepdims=True).astype(jnp.int32)
            slots[:, lanes_at(first, block)] = jnp.where(live, place, -1)
            offset = offset + jnp.sum(member, axis=1, keepdims=True)
        return offset

    lax.fori_loop(0, part_rows // wide, rank, jnp.concatenate(starts, axis=0))

    near[4].wait()
    near[5].wait()
    groups = ((0, 2), (2, values - 2))
    copies = []
    for at, (first_value, number) in enumerate(groups):
        mine = pl.ds(first_value, number)

        def place_values(b, carry, first_value=first_value, number=number, mine=mine):
            lanes = lanes_at(b * wide, wide)
            slot = slots[:, lanes]
            row = lax.shift_right_arithmetic(slot, int(math.log2(cols)))
            col = lax.bitwise_and(slot, cols - 1)
            taken = []
            for v in range(first_value, first_value + number):
                if v == 0:
                    taken.append((cell[:, lanes] + 1).astype(F32))
                else:
                    taken.append(volume[:, lanes] if v == 1 else drag[v - 2, :, lanes])
            sums = spread(taken, row, col, lines, cols).reshape(number, span_size, per, cols)
            packed[mine] += sums
            return carry

        packed[mine] = jnp.zeros((number, span_size, per, cols), F32)
        lax.fori_loop(0, part_rows // wide, place_values, 0)
        own = pltpu.make_async_copy(
            packed.at[mine, grid.span], recv.at[mine, grid.span], own_sem.at[at]
        )
        own.start()
        copies.append(own)
        for k in range(1, span_size):
            to = lax.rem(grid.span + k, span_size)
            copies.append(
                pltpu.make_async_remote_copy(
                    src_ref=packed.at[mine, to],
                    dst_ref=recv.at[mine, grid.span],
                    send_sem=send_sem.at[at, k],
                    recv_sem=recv_sem.at[at, k],
                    device_id=(to, grid.depth),
                    device_id_type=MESH,
                )
            )
            copies[-1].start()
    halo.forward()
    halo.arrive()
    for copy in copies:
        copy.wait()
    halo.sent()


def sweeps_kernel(
    solid, prior, prior_rows, prior_cols, target, out,
    source, first, second, middle, source_cols, middle_cols, send_sem, recv_sem,
):
    grid = Grid()
    comps, layers, width_x, width_y = target.shape
    total_x = width_x + 2 * RIM
    own = pl.ds(0, width_y)
    rest = pl.ds(width_y, LANES)
    own_rows = pl.ds(RIM, width_x)

    barrier = pltpu.get_barrier_semaphore()
    for dx, dy in X_STEPS + Y_STEPS:
        grid.signal(barrier, dx, dy)

    def halo_of(c, phase):
        buffer, cols_in = (source, source_cols) if phase == 0 else (middle, middle_cols)
        width = RIM - 1 if phase == 0 else RIM

        def rows_out(side):
            return buffer.at[c, pl.ds(RIM if side == 0 else RIM + width_x - width, width), :, own]

        def rows_in(side):
            return buffer.at[c, pl.ds(RIM - width if side == 0 else RIM + width_x, width), :, own]

        def rows_of(part):
            return pl.ds(*((RIM, width_x), (RIM - width, width), (RIM + width_x, width))[part])

        def edge(part, side):
            lanes = pl.ds(0 if side == 0 else width_y - LANES, LANES)
            return buffer.at[c, rows_of(part), :, lanes]

        def columns(part, side):
            return cols_in.at[c, side, rows_of(part)]

        return Halo(
            grid, rows_out, rows_in, edge, columns,
            lambda at: send_sem.at[c, phase, at], lambda at: recv_sem.at[c, phase, at],
        )

    halos = [[halo_of(c, phase) for phase in range(2)] for c in range(comps)]
    lane = lax.broadcasted_iota(jnp.int32, (1, layers, LANES), 2)

    def fill_cols(buffer, c, cols_in):
        buffer[c, :, :, rest] = jnp.where(lane < LANES // 2, cols_in[c, 1], cols_in[c, 0])

    for c in range(comps):
        for x in range(width_x):
            source[c, RIM + x, :, own] = target[c, :, x, :]
    for c in range(comps):
        field = solid if c == 0 else prior.at[c - 1]
        for x in range(width_x):
            first[c, RIM + x, :, own] = field[:, x, :]
        first[c, pl.ds(0, RIM), :, own] = prior_rows[c, 0]
        first[c, pl.ds(RIM + width_x, RIM), :, own] = prior_rows[c, 1]
        fill_cols(first, c, prior_cols)

    pl.semaphore_wait(barrier, grid.around(X_STEPS + Y_STEPS))
    for c in range(comps):
        halos[c][0].start()
    for side, at in ((0, 0), (1, RIM + width_x)):

        @pl.when(jnp.logical_not(grid.has(*X_STEPS[side])))
        def _(at=at):
            for buffer in (source, middle):
                zeros = jnp.zeros((comps, RIM, layers, width_y), F32)
                buffer[:, pl.ds(at, RIM), :, own] = zeros

        @pl.when(jnp.logical_not(grid.has(*Y_STEPS[side])))
        def _(side=side):
            for buffer in (source_cols, middle_cols):
                buffer[:, side] = jnp.zeros((comps, total_x, layers, LANES), F32)

    lanes = lax.broadcasted_iota(jnp.int32, (layers, width_y + LANES), 1)
    known = lanes < width_y
    known = known | ((lanes < width_y + LANES // 2) & (grid.depth < grid.depth_size - 1))
    known = known | ((lanes >= width_y + LANES // 2) & (grid.depth > 0))
    scale = jnp.where(known, 1.0 / (1.0 + 4.0 * NU_WEIGHT), 0.0)

    def relax(c, x, before, here, after):
        beside = before + after
        beside = beside + pltpu.roll(here, 1, 1) + pltpu.roll(here, width_y + LANES - 1, 1)
        return (source[c, x] + NU_WEIGHT * beside) * scale

    def sweep(c, old, new, gone):
        low, high = gone, total_x - gone
        step = max(k for k in range(1, 9) if (high - low) % k == 0)

        def rows(g, carry):
            before, here = carry
            for k in range(step):
                x = low + g * step + k
                after = old[c, x + 1]
                new[c, x] = relax(c, x, before, here, after)
                before, here = here, after
            return before, here

        lax.fori_loop(0, (high - low) // step, rows, (old[c, low - 1], old[c, low]))
        for side, x in ((0, RIM - 1), (1, RIM + width_x)):
            if low <= x < high:

                @pl.when(jnp.logical_not(grid.has(*X_STEPS[side])))
                def _(x=x):
                    new[c, x] = jnp.zeros((layers, width_y + LANES), F32)

    def first_half(c):
        halos[c][0].arrive()
        fill_cols(source, c, source_cols)
        sweep(c, first, second, 1)
        sweep(c, second, first, 2)
        sweep(c, first, middle, 3)
        halos[c][1].start()

    def second_half(c):
        halos[c][1].arrive()
        fill_cols(middle, c, middle_cols)
        sweep(c, middle, first, 1)
        sweep(c, first, second, 2)
        before, here = second[c, RIM - 1], second[c, RIM]
        for x in range(width_x):
            after = second[c, RIM + x + 1]
            out[c, :, x, :] = relax(c, RIM + x, before, here, after)[:, :width_y]
            before, here = here, after

    halos[0][0].forward()
    for c in range(comps):
        if c + 1 < comps:
            halos[c + 1][0].forward()
        first_half(c)
    halos[0][1].forward()
    for c in range(comps):
        if c + 1 < comps:
            halos[c + 1][1].forward()
        second_half(c)
    for c in range(comps):
        for phase in range(2):
            halos[c][phase].sent()


def feedback_kernel(wide, values, slots, out, table, hots, send_sem, recv_sem, own_sem):
    grid = Grid()
    comps, span_size, per, cols = values.shape
    lines = span_size * per
    part_rows = slots.shape[1]
    barrier = pltpu.get_barrier_semaphore()
    for k in range(1, span_size):
        to = lax.rem(grid.span + k, span_size)
        pl.semaphore_signal(barrier, inc=1, device_id=(to, grid.depth), device_id_type=MESH)
    def lanes_at(b):
        return pl.ds(pl.multiple_of(b * wide, wide), wide)

    def hot_step(b, carry):
        lanes = lanes_at(b)
        hots[:, lanes] = hot_at(lax.bitwise_and(slots[:, lanes], cols - 1), cols)
        return carry

    lax.fori_loop(0, part_rows // wide, hot_step, 0)
    pl.semaphore_wait(barrier, span_size - 1)
    groups = (pl.ds(0, comps // 2), pl.ds(comps // 2, comps - comps // 2))
    copies = []
    for at, mine in enumerate(groups):
        own = pltpu.make_async_copy(
            values.at[mine, grid.span], table.at[mine, grid.span], own_sem.at[at]
        )
        own.start()
        copies.append([own])
        for k in range(1, span_size):
            to = lax.rem(grid.span + k, span_size)
            copies[at].append(
                pltpu.make_async_remote_copy(
                    src_ref=values.at[mine, to],
                    dst_ref=table.at[mine, grid.span],
                    send_sem=send_sem.at[at, k],
                    recv_sem=recv_sem.at[at, k],
                    device_id=(to, grid.depth),
                    device_id_type=MESH,
                )
            )
            copies[at][-1].start()

    for at, mine in enumerate(groups):
        for copy in copies[at]:
            copy.wait()
        number = mine.size
        high, low = two_parts(table[mine].reshape(number * lines, cols))
        both = jnp.concatenate([high, low], axis=0)

        def pick_step(b, carry, mine=mine, number=number, both=both):
            lanes = lanes_at(b)
            row = lax.shift_right_arithmetic(slots[:, lanes], int(math.log2(cols)))
            wanted = lax.broadcasted_iota(jnp.int32, (lines, wide), 0) == row
            found = jnp.dot(both, hots[:, lanes], preferred_element_type=F32)
            for c in range(number):
                value = found[c * lines : (c + 1) * lines]
                value = value + found[(number + c) * lines : (number + c + 1) * lines]
                value = jnp.sum(jnp.where(wanted, value, 0.0), axis=0, keepdims=True)
                out[mine.start + c, :, lanes] = value
            return carry

        lax.fori_loop(0, part_rows // wide, pick_step, 0)


VMEM = pl.BlockSpec(memory_space=pltpu.VMEM)
SMEM = pl.BlockSpec(memory_space=pltpu.SMEM)
HBM = pl.BlockSpec(memory_space=pltpu.HBM)
LIMIT = pltpu.CompilerParams(vmem_limit_bytes=48 * 1024 * 1024)


def far(number):
    return pltpu.CompilerParams(
        vmem_limit_bytes=48 * 1024 * 1024, collective_id=number, has_side_effects=True
    )


def on_device(part_slab, part_cell, part_volume, part_drag, part_count, prior_solid, prior_drag):
    span_size = lax.axis_size("span")
    part_rows = part_cell.shape[1]
    cap = 2 * part_rows // span_size
    layers, width_x, width_y = prior_solid.shape
    cols = min(256, cap)
    lines = span_size * cap // cols
    per = lines // span_size
    block = math.gcd(part_rows, 512)
    wide = math.gcd(part_rows, 2048)
    total_x = width_x + 2 * RIM
    dma = pltpu.SemaphoreType.DMA
    recv, slots, prior_rows, prior_cols = pl.pallas_call(
        functools.partial(
            collect_kernel, cap, block, wide, layers, int(math.log2(width_x * width_y))
        ),
        out_shape=(
            jax.ShapeDtypeStruct((5, span_size, per, cols), F32),
            jax.ShapeDtypeStruct((1, part_rows), jnp.int32),
            jax.ShapeDtypeStruct((4, 2, RIM, layers, width_y), F32),
            jax.ShapeDtypeStruct((4, 2, total_x, layers, LANES), F32),
        ),
        in_specs=[SMEM] + [HBM] * 6,
        out_specs=(VMEM,) * 4,
        scratch_shapes=[
            pltpu.VMEM((5, span_size, per, cols), F32),
            pltpu.VMEM((4, 2, RIM, layers, width_y), F32),
            pltpu.VMEM((4, 2, width_x, layers, LANES), F32),
            pltpu.VMEM((1, part_rows), jnp.int32),
            pltpu.VMEM((1, part_rows), jnp.int32),
            pltpu.VMEM((1, part_rows), F32),
            pltpu.VMEM(part_drag.shape, F32),
            pltpu.VMEM(prior_solid.shape, F32),
            pltpu.VMEM(prior_drag.shape, F32),
            dma((HALO_COPIES,)),
            dma((HALO_COPIES,)),
            dma((2, span_size)),
            dma((2, span_size)),
            dma((2,)),
            dma((6,)),
        ],
        compiler_params=far(1),
        name="collect",
    )(
        part_count,
        *[
            pltpu.with_memory_space_constraint(a, pltpu.HBM)
            for a in (
                part_slab.reshape(1, part_rows), part_cell, part_volume, part_drag,
                prior_solid, prior_drag,
            )
        ],
    )
    recv = recv.reshape(5, lines, cols)
    bins = Bins(layers, width_x, width_y, span_size, lines, cols)
    target = pl.pallas_call(
        functools.partial(deposit_kernel, bins),
        out_shape=jax.ShapeDtypeStruct((4, layers, width_x, width_y), F32),
        in_specs=[VMEM],
        out_specs=VMEM,
        compiler_params=LIMIT,
        name="deposit",
    )(recv)
    whole = pltpu.VMEM((4, total_x, layers, width_y + LANES), F32)
    columns = pltpu.VMEM((4, 2, total_x, layers, LANES), F32)
    smooth = pl.pallas_call(
        sweeps_kernel,
        out_shape=jax.ShapeDtypeStruct(target.shape, F32),
        in_specs=[VMEM] * 5,
        out_specs=VMEM,
        scratch_shapes=[whole] * 4 + [columns] * 2 + [dma((4, 2, HALO_COPIES))] * 2,
        compiler_params=far(0),
        name="sweeps",
    )(prior_solid, prior_drag, prior_rows, prior_cols, target)
    fields, values = pl.pallas_call(
        functools.partial(gather_kernel, bins),
        out_shape=(
            jax.ShapeDtypeStruct((4, layers, width_x, width_y), F32),
            jax.ShapeDtypeStruct((4, lines, cols), F32),
        ),
        in_specs=[VMEM] * 2,
        out_specs=(VMEM, VMEM),
        scratch_shapes=[pltpu.VMEM((layers, 8 * bins.rows, bins.cols), BF)],
        compiler_params=LIMIT,
        name="gather",
    )(smooth, recv)
    feedback = pl.pallas_call(
        functools.partial(feedback_kernel, wide),
        out_shape=jax.ShapeDtypeStruct((4, 1, part_rows), F32),
        in_specs=[VMEM] * 2,
        out_specs=VMEM,
        scratch_shapes=[
            pltpu.VMEM((4, span_size, per, cols), F32),
            pltpu.VMEM((cols, part_rows), BF),
            dma((2, span_size)),
            dma((2, span_size)),
            dma((2,)),
        ],
        compiler_params=far(2),
        name="feedback",
    )(values.reshape(4, span_size, per, cols), slots)
    return (fields, feedback)


def solution(mesh):
    in_specs = (
        P("depth", "span", None),
        P("depth", "span"),
        P("depth", "span"),
        P(None, "depth", "span"),
        P("depth", "span"),
        P(None, "span", "depth"),
        P(None, None, "span", "depth"),
    )
    out_specs = (P(None, None, "span", "depth"), P(None, "depth", "span"))
    return jax.shard_map(
        on_device, mesh=mesh, in_specs=in_specs, out_specs=out_specs, check_vma=False
    )
```

```python
import functools
import math

import jax
import jax.numpy as jnp
from jax import lax
from jax.experimental import pallas as pl
from jax.experimental.pallas import tpu as pltpu
from jax.sharding import PartitionSpec as P

SWEEPS = 6
NU_WEIGHT = 1.0
PHI_LIMIT = 0.6
BF = jnp.bfloat16
F32 = jnp.float32


def two_parts(value):
    high = value.astype(BF)
    return high, (value - high.astype(F32)).astype(BF)


def nt_dot(left, right):
    return lax.dot_general(left, right, (((1,), (1,)), ((), ())), preferred_element_type=F32)


def hot_at(index, count):
    rows = lax.broadcasted_iota(jnp.int32, (count, index.shape[1]), 0)
    return jnp.where(rows == index, 1.0, 0.0).astype(BF)


def spread(values, row, col, rows, cols):
    mask = hot_at(row, rows)
    parts = [two_parts(v) for v in values]
    left = jnp.concatenate([mask * p[k] for k in range(2) for p in parts], axis=0)
    both = nt_dot(left, hot_at(col, cols))
    n = len(values) * rows
    return both[:n] + both[n:]


class Bins:
    def __init__(self, layers, width_x, width_y, span, lines, cols):
        self.layers, self.span, self.lines, self.line = layers, span, lines, cols
        self.binned = lines == span * layers
        self.cols = min(256, width_y)
        self.parts = width_y // self.cols
        self.rows = width_x * self.parts
        self.width_x, self.width_y = width_x, width_y
        self.log_y, self.log_cols = int(math.log2(width_y)), int(math.log2(self.cols))
        self.log_x = int(math.log2(width_x))

    def place(self, ids):
        y = lax.bitwise_and(ids, self.width_y - 1)
        x = lax.bitwise_and(lax.shift_right_arithmetic(ids, self.log_y), self.width_x - 1)
        row = lax.shift_right_arithmetic(y, self.log_cols) * self.width_x + x
        return self.layer(ids) * self.rows + row, lax.bitwise_and(y, self.cols - 1)

    def layer(self, ids):
        return lax.shift_right_arithmetic(ids, self.log_x + self.log_y)

    def strays(self, ids, line, lane):
        live = ids >= 0
        if not self.binned:
            return live
        own = lax.rem(line, self.layers)
        layer = self.layer(ids)
        beside = jnp.where(lane < self.line // 2, own - 1, own + 1)
        return live & (layer != own) & (layer != beside)

    def any_stray(self, ref):
        ids = ref[0].astype(jnp.int32) - 1
        line, lane = (lax.broadcasted_iota(jnp.int32, ids.shape, axis) for axis in range(2))
        mask = self.strays(ids, line, lane)
        return jnp.max(jnp.where(mask, 1.0, 0.0)) > 0.0

    def pieces(self, j):
        half = self.line // 2
        return [
            (pl.ds(o * self.layers + j, 1), slice(h * half, (h + 1) * half))
            for h in range(2)
            for o in range(self.span)
        ]

    def flat(self, ref, c, j):
        return jnp.concatenate([ref[c, line, lanes] for line, lanes in self.pieces(j)], axis=1)

    def group(self, ref, c, g):
        block = ref[c, pl.ds(pl.multiple_of(g * 8, 8), 8), :]
        return jnp.concatenate([block[k : k + 1] for k in range(8)], axis=1)

    def stray_group(self, ref, g):
        ids = self.group(ref, 0, g).astype(jnp.int32) - 1
        lane = lax.broadcasted_iota(jnp.int32, ids.shape, 1)
        shift = int(math.log2(self.line))
        line = g * 8 + lax.shift_right_arithmetic(lane, shift)
        return ids, self.strays(ids, line, lax.bitwise_and(lane, self.line - 1))


def deposit_kernel(bins, recv, out):
    comps = out.shape[0]
    rows, cols, width_x = bins.rows, bins.cols, bins.width_x
    out[...] = jnp.zeros_like(out)

    def add(layer, sums):
        for c in range(comps):
            for part in range(bins.parts):
                lanes = slice(part * cols, (part + 1) * cols)
                first = c * rows + part * width_x
                out[c, layer, :, lanes] += sums[first : first + width_x]

    if bins.binned:

        for j in range(bins.layers):
            flat = [bins.flat(recv, c, j) for c in range(comps + 1)]
            ids = flat[0].astype(jnp.int32) - 1
            place, col = bins.place(ids)
            hot = hot_at(col, cols)
            parts = [two_parts(v) for v in flat[1:]]
            n = ids.shape[1] // 2

            def sums(layer, lanes, place=place, parts=parts, hot=hot):
                mask = hot_at(place[:, lanes] - layer * rows, rows)
                left = [mask * p[k][:, lanes] for k in range(2) for p in parts]
                both = nt_dot(jnp.concatenate(left, axis=0), hot[:, lanes])
                return both[: comps * rows] + both[comps * rows :]

            add(j, sums(j, slice(0, 2 * n)))
            if j > 0:
                add(j - 1, sums(j - 1, slice(0, n)))
            if j < bins.layers - 1:
                add(j + 1, sums(j + 1, slice(n, 2 * n)))

    @pl.when(bins.any_stray(recv))
    def _():
        def line_step(g, carry):
            ids, mask = bins.stray_group(recv, g)
            place, col = bins.place(ids)
            values = [jnp.where(mask, bins.group(recv, 1 + c, g), 0.0) for c in range(comps)]

            def layer_step(layer, inner):
                add(layer, spread(values, place - layer * rows, col, rows, cols))
                return inner

            return lax.fori_loop(0, bins.layers, layer_step, carry)

        lax.fori_loop(0, bins.lines // 8, line_step, 0)

    out[0] = jnp.minimum(out[0], PHI_LIMIT)


def fill_table(bins, table, fields):
    comps = len(fields)
    for c, value in enumerate(fields):
        high, low = two_parts(value)
        for part in range(bins.parts):
            lanes = slice(part * bins.cols, (part + 1) * bins.cols)
            first = c * bins.rows + part * bins.width_x
            table[pl.ds(first, bins.width_x)] = high[:, lanes]
            table[pl.ds(comps * bins.rows + first, bins.width_x)] = low[:, lanes]


def fields_of(smooth, layer, comps):
    void = 1.0 - smooth[0, layer]
    return [void if c == 0 else -smooth[c, layer] / void for c in comps]


def near_values(bins, tables, ids_ref, lines, out):
    rows, cols, half = bins.rows, bins.cols, bins.line // 2
    height = tables.shape[1]
    comps = height // (2 * rows)
    for j in lines:
        for h in range(2):
            lanes = slice(h * half, (h + 1) * half)
            ids = [ids_ref[0, pl.ds(o * bins.layers + j, 1), lanes] for o in range(bins.span)]
            ids = jnp.concatenate(ids, axis=1).astype(jnp.int32) - 1
            place, col = bins.place(ids)
            low, high = max(j - 1 + h, 0), min(j + h, bins.layers - 1)
            number = high - low + 1
            table = tables[low : high + 1].reshape(number * height, cols)
            wide = jnp.dot(table, hot_at(col, cols), preferred_element_type=F32)
            row = lax.broadcasted_iota(jnp.int32, (rows, ids.shape[1]), 0)
            here = [row == place - layer * rows for layer in range(low, high + 1)]
            for c in range(comps):
                found = 0.0
                for k in range(number):
                    first = k * height + c * rows
                    second = first + comps * rows
                    value = wide[first : first + rows] + wide[second : second + rows]
                    found = jnp.where(here[k], value, found)
                found = jnp.sum(found, axis=0, keepdims=True)
                for o in range(bins.span):
                    out(c, o, j, lanes, found[:, o * half : (o + 1) * half])


def fields_kernel(bins, smooth, ids_ref, fields, early_tables, late_tables, out, tables):
    comps = smooth.shape[0]
    rows, cols = bins.rows, bins.cols
    early = comps // 2

    def table_step(layer, carry):
        values = fields_of(smooth, layer, range(comps))
        for c in range(comps):
            fields[c, layer] = values[c]
        fill_table(bins, early_tables.at[layer], values[:early])
        fill_table(bins, late_tables.at[layer], values[early:])
        return carry

    lax.fori_loop(0, bins.layers, table_step, 0)
    out[...] = jnp.zeros_like(out)

    @pl.when(bins.any_stray(ids_ref))
    def _():
        def all_step(layer, carry):
            fill_table(bins, tables.at[layer], [fields[c, layer] for c in range(comps)])
            return carry

        lax.fori_loop(0, bins.layers, all_step, 0)

        def line_step(g, carry):
            ids, mask = bins.stray_group(ids_ref, g)
            place, col = bins.place(ids)
            hot = hot_at(col, cols)
            row = lax.broadcasted_iota(jnp.int32, (rows, ids.shape[1]), 0)

            def layer_step(layer, total):
                wide = jnp.dot(tables[layer], hot, preferred_element_type=F32)
                here = (row == place - layer * rows) & mask
                more = []
                for c in range(comps):
                    second = (comps + c) * rows
                    value = wide[c * rows : (c + 1) * rows] + wide[second : second + rows]
                    value = jnp.where(here, value, 0.0)
                    more.append(total[c] + jnp.sum(value, axis=0, keepdims=True))
                return more

            zero = [jnp.zeros(ids.shape, F32)] * comps
            total = lax.fori_loop(0, bins.layers, layer_step, zero)
            n = bins.line
            for c in range(comps):
                block = [total[c][:, k * n : (k + 1) * n] for k in range(8)]
                out[c, pl.ds(pl.multiple_of(g * 8, 8), 8), :] = jnp.concatenate(block, axis=0)
            return carry

        lax.fori_loop(0, bins.lines // 8, line_step, 0)


MESH = pl.DeviceIdType.MESH
RIM = SWEEPS // 2
LANES = 128


class Grid:
    def __init__(self):
        self.span, self.depth = lax.axis_index("span"), lax.axis_index("depth")
        self.span_size, self.depth_size = lax.axis_size("span"), lax.axis_size("depth")

    def has(self, dx, dy):
        x, y = self.span + dx, self.depth + dy
        return (x >= 0) & (x < self.span_size) & (y >= 0) & (y < self.depth_size)

    def peer(self, dx, dy):
        return (self.span + dx, self.depth + dy)

    def signal(self, barrier, dx, dy):
        @pl.when(self.has(dx, dy))
        def _():
            pl.semaphore_signal(barrier, inc=1, device_id=self.peer(dx, dy), device_id_type=MESH)

    def around(self, steps):
        return sum(self.has(dx, dy).astype(jnp.int32) for dx, dy in steps)


X_STEPS = ((-1, 0), (1, 0))
Y_STEPS = ((0, -1), (0, 1))


class Halo:
    def __init__(self, grid, rows_out, rows_in, edge, columns, send_sem, recv_sem):
        self.grid = grid
        self.rows_out, self.rows_in, self.edge, self.columns = rows_out, rows_in, edge, columns
        self.send_sem, self.recv_sem = send_sem, recv_sem

    def _copy(self, src, dst, at, step):
        return pltpu.make_async_remote_copy(
            src_ref=src,
            dst_ref=dst,
            send_sem=self.send_sem(at),
            recv_sem=self.recv_sem(at),
            device_id=self.grid.peer(*step),
            device_id_type=MESH,
        )

    def rows(self, side):
        return self._copy(self.rows_out(side), self.rows_in(1 - side), side, X_STEPS[side])

    def cols(self, part, side):
        at = 2 + 2 * part + side
        return self._copy(self.edge(part, side), self.columns(part, 1 - side), at, Y_STEPS[side])

    def _when(self, step, action):
        @pl.when(self.grid.has(*step))
        def _():
            action()

    def start(self):
        for side in range(2):
            self._when(X_STEPS[side], lambda: self.rows(side).start())
        self.start_cols((0,))

    def start_cols(self, parts):
        for part in parts:
            for side in range(2):
                self._when(Y_STEPS[side], lambda: self.cols(part, side).start())

    def rows_arrive(self):
        for side in range(2):
            self._when(X_STEPS[1 - side], lambda: self.rows(side).wait_recv())

    def forward(self):
        self.rows_arrive()
        self.start_cols((1, 2))

    def arrive(self, parts=(0, 1, 2)):
        for part in parts:
            for side in range(2):
                self._when(Y_STEPS[1 - side], lambda: self.cols(part, side).wait_recv())

    def rows_sent(self):
        for side in range(2):
            self._when(X_STEPS[side], lambda: self.rows(side).wait_send())

    def cols_sent(self, parts=(0, 1, 2)):
        for part in parts:
            for side in range(2):
                self._when(Y_STEPS[side], lambda: self.cols(part, side).wait_send())

    def sent(self):
        self.rows_sent()
        self.cols_sent()


HALO_COPIES = 8


def collect_kernel(
    cap, block, wide, layers, shift, count, slab_far, cell_far, volume_far, drag_far, solid_far,
    prior_far, recv, slots, rows_in, cols_in, packed, rows_out, cols_out,
    slab, cell, volume, drag, solid, prior, halo_send, halo_recv, send_sem, recv_sem, own_sem,
    near_sem,
):
    pairs = (
        (slab_far, slab), (cell_far, cell), (solid_far, solid), (prior_far, prior),
        (volume_far, volume), (drag_far, drag),
    )
    near = [pltpu.make_async_copy(a, b, near_sem.at[k]) for k, (a, b) in enumerate(pairs)]
    for copy in near:
        copy.start()
    grid = Grid()
    span_size = grid.span_size
    values, _, per, cols = recv.shape
    lines = span_size * per
    part_rows = slab.shape[1]
    width_x, width_y = solid.shape[1:]
    comps = 1 + prior.shape[0]

    barrier = pltpu.get_barrier_semaphore()
    for k in range(1, span_size):
        to = lax.rem(grid.span + k, span_size)
        pl.semaphore_signal(barrier, inc=1, device_id=(to, grid.depth), device_id_type=MESH)
    for dx, dy in Y_STEPS:
        grid.signal(barrier, dx, dy)

    keys = layers * span_size
    live_count = count[0, 0]
    many = wide // block

    def lanes_at(first, size):
        return pl.ds(pl.multiple_of(first, size), size)

    def member_of(first):
        lanes = lanes_at(first, block)
        live = first + lax.broadcasted_iota(jnp.int32, (1, block), 1) < live_count
        layer = lax.shift_right_arithmetic(cell[:, lanes], shift)
        key = jnp.where(live, layer * span_size + slab[:, lanes], -1)
        member = jnp.where(lax.broadcasted_iota(jnp.int32, (keys, block), 0) == key, 1.0, 0.0)
        return member, live

    fold = min(block, LANES)

    def tally(b, total):
        for m in range(many):
            member = member_of(b * wide + m * block)[0]
            for k in range(block // fold):
                total = total + member[:, k * fold : (k + 1) * fold]
        return total

    near[0].wait()
    near[1].wait()
    total = lax.fori_loop(0, part_rows // wide, tally, jnp.zeros((keys, fold), F32))
    near[2].wait()
    near[3].wait()
    for c in range(comps):
        field = solid if c == 0 else prior.at[c - 1]
        for x in range(width_x):
            line = field[:, x, :]
            if x < RIM:
                rows_out[c, 0, x] = line
            if x >= width_x - RIM:
                rows_out[c, 1, x - width_x + RIM] = line
            cols_out[c, 0, x] = line[:, :LANES]
            cols_out[c, 1, x] = line[:, width_y - LANES :]
    for side in range(2):

        @pl.when(jnp.logical_not(grid.has(*X_STEPS[side])))
        def _(side=side):
            rows_in[:, side] = jnp.zeros((comps, RIM, layers, width_y), F32)

        @pl.when(jnp.logical_not(grid.has(*Y_STEPS[side])))
        def _(side=side):
            cols_in[:, side] = jnp.zeros((comps, width_x, layers, LANES), F32)

    halo = Halo(
        grid, lambda side: rows_out.at[:, side], lambda side: rows_in.at[:, side],
        lambda part, side: cols_out.at[:, side], lambda part, side: cols_in.at[:, side],
        lambda at: halo_send.at[at], lambda at: halo_recv.at[at],
    )
    pl.semaphore_wait(barrier, span_size - 1 + grid.around(Y_STEPS))
    halo.start()

    before_lane = lax.broadcasted_iota(jnp.int32, (block, block), 0)
    this_lane = lax.broadcasted_iota(jnp.int32, (block, block), 1)
    tri = jnp.where(before_lane < this_lane, 1.0, 0.0).astype(BF)
    total = jnp.sum(total, axis=1, keepdims=True)
    counts = [total[k * span_size : (k + 1) * span_size] for k in range(layers)]
    rest = [None] * layers
    left = jnp.zeros((span_size, 1), F32)
    for k in reversed(range(layers)):
        left = left + counts[k]
        rest[k] = left
    base = lax.broadcasted_iota(jnp.int32, (span_size, 1), 0).astype(F32) * cap
    end = jnp.zeros((span_size, 1), F32)
    starts = []
    for k in range(layers):
        start = jnp.minimum(jnp.maximum(end, float(cap // layers * k)), cap - rest[k])
        starts.append(start + base)
        end = start + counts[k]

    def rank(b, offset):
        for m in range(many):
            first = b * wide + m * block
            member, live = member_of(first)
            before = jnp.dot(member.astype(BF), tri, preferred_element_type=F32)
            place = jnp.sum(member * (before + offset), axis=0, keepdims=True).astype(jnp.int32)
            slots[:, lanes_at(first, block)] = jnp.where(live, place, -1)
            offset = offset + jnp.sum(member, axis=1, keepdims=True)
        return offset

    lax.fori_loop(0, part_rows // wide, rank, jnp.concatenate(starts, axis=0))

    near[4].wait()
    near[5].wait()
    groups = ((0, 2), (2, values - 2))
    copies = []
    for at, (first_value, number) in enumerate(groups):
        mine = pl.ds(first_value, number)

        def place_values(b, carry, first_value=first_value, number=number, mine=mine):
            lanes = lanes_at(b * wide, wide)
            slot = slots[:, lanes]
            row = lax.shift_right_arithmetic(slot, int(math.log2(cols)))
            col = lax.bitwise_and(slot, cols - 1)
            taken = []
            for v in range(first_value, first_value + number):
                if v == 0:
                    taken.append((cell[:, lanes] + 1).astype(F32))
                else:
                    taken.append(volume[:, lanes] if v == 1 else drag[v - 2, :, lanes])
            sums = spread(taken, row, col, lines, cols).reshape(number, span_size, per, cols)
            packed[mine] += sums
            return carry

        packed[mine] = jnp.zeros((number, span_size, per, cols), F32)
        lax.fori_loop(0, part_rows // wide, place_values, 0)
        own = pltpu.make_async_copy(
            packed.at[mine, grid.span], recv.at[mine, grid.span], own_sem.at[at]
        )
        own.start()
        copies.append(own)
        for k in range(1, span_size):
            to = lax.rem(grid.span + k, span_size)
            copies.append(
                pltpu.make_async_remote_copy(
                    src_ref=packed.at[mine, to],
                    dst_ref=recv.at[mine, grid.span],
                    send_sem=send_sem.at[at, k],
                    recv_sem=recv_sem.at[at, k],
                    device_id=(to, grid.depth),
                    device_id_type=MESH,
                )
            )
            copies[-1].start()
    for copy in copies:
        copy.wait()
    halo.rows_arrive()
    halo.arrive((0,))
    halo.rows_sent()
    halo.cols_sent((0,))


def sweeps_kernel(
    bins, solid, prior, prior_rows, prior_cols, target, ids_ref, out, early_values,
    source, first, second, middle, source_cols, middle_cols, corners, tables, send_sem, recv_sem,
    corner_send, corner_recv,
):
    grid = Grid()
    comps, layers, width_x, width_y = target.shape
    total_x = width_x + 2 * RIM
    own = pl.ds(0, width_y)
    rest = pl.ds(width_y, LANES)
    own_rows = pl.ds(RIM, width_x)

    barrier = pltpu.get_barrier_semaphore()
    for dx, dy in X_STEPS + Y_STEPS:
        grid.signal(barrier, dx, dy)

    def halo_of(c, phase):
        buffer, cols_in = (source, source_cols) if phase == 0 else (middle, middle_cols)
        width = RIM - 1 if phase == 0 else RIM

        def rows_out(side):
            return buffer.at[c, pl.ds(RIM if side == 0 else RIM + width_x - width, width), :, own]

        def rows_in(side):
            return buffer.at[c, pl.ds(RIM - width if side == 0 else RIM + width_x, width), :, own]

        def rows_of(part):
            return pl.ds(*((RIM, width_x), (RIM - width, width), (RIM + width_x, width))[part])

        def edge(part, side):
            lanes = pl.ds(0 if side == 0 else width_y - LANES, LANES)
            return buffer.at[c, rows_of(part), :, lanes]

        def columns(part, side):
            return cols_in.at[c, side, rows_of(part)]

        return Halo(
            grid, rows_out, rows_in, edge, columns,
            lambda at: send_sem.at[c, phase, at], lambda at: recv_sem.at[c, phase, at],
        )

    def corner_edge(part, side):
        lanes = pl.ds(0 if side == 0 else width_y - LANES, LANES)
        return prior_rows.at[:, part - 1, :, :, lanes]

    around = Halo(
        grid, None, None, corner_edge, lambda part, side: corners.at[:, side, part - 1],
        lambda at: corner_send.at[at], lambda at: corner_recv.at[at],
    )
    halos = [[halo_of(c, phase) for phase in range(2)] for c in range(comps)]
    lane = lax.broadcasted_iota(jnp.int32, (1, layers, LANES), 2)

    def fill_cols(buffer, c, cols_in):
        buffer[c, :, :, rest] = jnp.where(lane < LANES // 2, cols_in[c, 1], cols_in[c, 0])

    for c in range(comps):
        for x in range(width_x):
            source[c, RIM + x, :, own] = target[c, :, x, :]
    for c in range(comps):
        field = solid if c == 0 else prior.at[c - 1]
        for x in range(width_x):
            first[c, RIM + x, :, own] = field[:, x, :]
        first[c, pl.ds(0, RIM), :, own] = prior_rows[c, 0]
        first[c, pl.ds(RIM + width_x, RIM), :, own] = prior_rows[c, 1]
        first[c, own_rows, :, rest] = jnp.where(lane < LANES // 2, prior_cols[c, 1], prior_cols[c, 0])

    pl.semaphore_wait(barrier, grid.around(X_STEPS + Y_STEPS))
    for c in range(comps):
        halos[c][0].start()
    around.start_cols((1, 2))
    for side, at in ((0, 0), (1, RIM + width_x)):

        @pl.when(jnp.logical_not(grid.has(*X_STEPS[side])))
        def _(at=at):
            for buffer in (source, middle):
                zeros = jnp.zeros((comps, RIM, layers, width_y), F32)
                buffer[:, pl.ds(at, RIM), :, own] = zeros

        @pl.when(jnp.logical_not(grid.has(*Y_STEPS[side])))
        def _(side=side):
            for buffer in (source_cols, middle_cols):
                buffer[:, side] = jnp.zeros((comps, total_x, layers, LANES), F32)
            corners[:, side] = jnp.zeros((comps, 2, RIM, layers, LANES), F32)

    lanes = lax.broadcasted_iota(jnp.int32, (layers, width_y + LANES), 1)
    known = lanes < width_y
    known = known | ((lanes < width_y + LANES // 2) & (grid.depth < grid.depth_size - 1))
    known = known | ((lanes >= width_y + LANES // 2) & (grid.depth > 0))
    scale = jnp.where(known, 1.0 / (1.0 + 4.0 * NU_WEIGHT), 0.0)

    def relax(c, x, before, here, after):
        beside = before + after
        beside = beside + pltpu.roll(here, 1, 1) + pltpu.roll(here, width_y + LANES - 1, 1)
        return (source[c, x] + NU_WEIGHT * beside) * scale

    def sweep(c, old, new, gone):
        low, high = gone, total_x - gone
        step = max(k for k in range(1, 9) if (high - low) % k == 0)

        def rows(g, carry):
            before, here = carry
            for k in range(step):
                x = low + g * step + k
                after = old[c, x + 1]
                new[c, x] = relax(c, x, before, here, after)
                before, here = here, after
            return before, here

        lax.fori_loop(0, (high - low) // step, rows, (old[c, low - 1], old[c, low]))
        for side, x in ((0, RIM - 1), (1, RIM + width_x)):
            if low <= x < high:

                @pl.when(jnp.logical_not(grid.has(*X_STEPS[side])))
                def _(x=x):
                    new[c, x] = jnp.zeros((layers, width_y + LANES), F32)

    def first_half(c):
        halos[c][0].arrive()
        fill_cols(source, c, source_cols)
        sweep(c, first, second, 1)
        sweep(c, second, first, 2)
        sweep(c, first, middle, 3)
        halos[c][1].start()

    def second_half(c):
        halos[c][1].arrive()
        fill_cols(middle, c, middle_cols)
        sweep(c, middle, first, 1)
        sweep(c, first, second, 2)
        before, here = second[c, RIM - 1], second[c, RIM]
        for x in range(width_x):
            after = second[c, RIM + x + 1]
            out[c, :, x, :] = relax(c, RIM + x, before, here, after)[:, :width_y]
            before, here = here, after

    around.arrive((1, 2))
    for c in range(comps):
        for part, at in ((0, 0), (1, RIM + width_x)):
            first[c, pl.ds(at, RIM), :, rest] = jnp.where(
                lane < LANES // 2, corners[c, 1, part], corners[c, 0, part]
            )
    halos[0][0].forward()
    for c in range(comps):
        if c + 1 < comps:
            halos[c + 1][0].forward()
        first_half(c)
    early = early_values.shape[0]
    parts = comps - early

    early_values[...] = jnp.zeros_like(early_values)

    def put(c, owner, line, lanes, value):
        early_values[c, owner, pl.ds(line, 1), lanes] = value

    halos[0][1].forward()
    for c in range(comps):
        if c + 1 < comps:
            halos[c + 1][1].forward()
        second_half(c)
        if not bins.binned:
            continue
        if c == early - 1:

            def table_step(layer, carry):
                fill_table(bins, tables.at[layer], fields_of(out, layer, range(early)))
                return carry

            lax.fori_loop(0, layers, table_step, 0)
        if early - 1 <= c < comps - 1:
            at = c - early + 1
            share = layers // (2 * parts)
            lines = range(share * at, share * (at + 1))
            near_values(bins, tables, ids_ref, lines, put)
    for c in range(comps):
        for phase in range(2):
            halos[c][phase].sent()
    around.cols_sent((1, 2))


def feedback_kernel(
    bins, wide, ids_ref, early_values, early_tables, late_tables, strays, slots, out,
    values, table, hots, send_sem, recv_sem, own_sem,
):
    grid = Grid()
    comps, span_size, per, cols = values.shape
    lines = span_size * per
    part_rows = slots.shape[1]
    early = early_values.shape[0]
    barrier = pltpu.get_barrier_semaphore()
    for k in range(1, span_size):
        to = lax.rem(grid.span + k, span_size)
        pl.semaphore_signal(barrier, inc=1, device_id=(to, grid.depth), device_id_type=MESH)

    def put(c, owner, line, lanes, value):
        more = strays[early + c, owner, pl.ds(line, 1), lanes]
        values[early + c, owner, pl.ds(line, 1), lanes] = value + more

    def put_early(c, owner, line, lanes, value):
        more = strays[c, owner, pl.ds(line, 1), lanes]
        values[c, owner, pl.ds(line, 1), lanes] = value + more

    values[pl.ds(0, early)] = early_values[...] + strays[pl.ds(0, early)]
    copies = []

    def send(first, number):
        mine = pl.ds(first, number)
        at = len(copies)
        started = [
            pltpu.make_async_copy(
                values.at[mine, grid.span], table.at[mine, grid.span], own_sem.at[at]
            )
        ]
        for k in range(1, span_size):
            to = lax.rem(grid.span + k, span_size)
            started.append(
                pltpu.make_async_remote_copy(
                    src_ref=values.at[mine, to],
                    dst_ref=table.at[mine, grid.span],
                    send_sem=send_sem.at[at, k],
                    recv_sem=recv_sem.at[at, k],
                    device_id=(to, grid.depth),
                    device_id_type=MESH,
                )
            )
        for copy in started:
            copy.start()
        copies.append((mine, started))

    half = bins.layers // 2
    if bins.binned:
        near_values(bins, early_tables, ids_ref, range(half, bins.layers), put_early)
    else:
        values[pl.ds(early, comps - early)] = strays[pl.ds(early, comps - early)]
    pl.semaphore_wait(barrier, span_size - 1)
    send(0, early)
    if bins.binned:
        near_values(bins, late_tables, ids_ref, range(bins.layers), put)
    send(early, comps - early)

    def lanes_at(b):
        return pl.ds(pl.multiple_of(b * wide, wide), wide)

    def hot_step(b, carry):
        lanes = lanes_at(b)
        hots[:, lanes] = hot_at(lax.bitwise_and(slots[:, lanes], cols - 1), cols)
        return carry

    lax.fori_loop(0, part_rows // wide, hot_step, 0)
    for mine, started in copies:
        for copy in started:
            copy.wait()
        number = mine.size
        high, low = two_parts(table[mine].reshape(number * lines, cols))
        both = jnp.concatenate([high, low], axis=0)

        def pick_step(b, carry, mine=mine, number=number, both=both):
            lanes = lanes_at(b)
            row = lax.shift_right_arithmetic(slots[:, lanes], int(math.log2(cols)))
            wanted = lax.broadcasted_iota(jnp.int32, (lines, wide), 0) == row
            found = jnp.dot(both, hots[:, lanes], preferred_element_type=F32)
            for c in range(number):
                value = found[c * lines : (c + 1) * lines]
                value = value + found[(number + c) * lines : (number + c + 1) * lines]
                value = jnp.sum(jnp.where(wanted, value, 0.0), axis=0, keepdims=True)
                out[mine.start + c, :, lanes] = value
            return carry

        lax.fori_loop(0, part_rows // wide, pick_step, 0)


VMEM = pl.BlockSpec(memory_space=pltpu.VMEM)
SMEM = pl.BlockSpec(memory_space=pltpu.SMEM)
HBM = pl.BlockSpec(memory_space=pltpu.HBM)
LIMIT = pltpu.CompilerParams(vmem_limit_bytes=48 * 1024 * 1024)


def far(number):
    return pltpu.CompilerParams(
        vmem_limit_bytes=48 * 1024 * 1024, collective_id=number, has_side_effects=True
    )


def on_device(part_slab, part_cell, part_volume, part_drag, part_count, prior_solid, prior_drag):
    span_size = lax.axis_size("span")
    part_rows = part_cell.shape[1]
    cap = 2 * part_rows // span_size
    layers, width_x, width_y = prior_solid.shape
    cols = min(256, cap)
    lines = span_size * cap // cols
    per = lines // span_size
    block = math.gcd(part_rows, 512)
    wide = math.gcd(part_rows, 2048)
    total_x = width_x + 2 * RIM
    dma = pltpu.SemaphoreType.DMA
    recv, slots, prior_rows, prior_cols = pl.pallas_call(
        functools.partial(
            collect_kernel, cap, block, wide, layers, int(math.log2(width_x * width_y))
        ),
        out_shape=(
            jax.ShapeDtypeStruct((5, span_size, per, cols), F32),
            jax.ShapeDtypeStruct((1, part_rows), jnp.int32),
            jax.ShapeDtypeStruct((4, 2, RIM, layers, width_y), F32),
            jax.ShapeDtypeStruct((4, 2, width_x, layers, LANES), F32),
        ),
        in_specs=[SMEM] + [HBM] * 6,
        out_specs=(VMEM,) * 4,
        scratch_shapes=[
            pltpu.VMEM((5, span_size, per, cols), F32),
            pltpu.VMEM((4, 2, RIM, layers, width_y), F32),
            pltpu.VMEM((4, 2, width_x, layers, LANES), F32),
            pltpu.VMEM((1, part_rows), jnp.int32),
            pltpu.VMEM((1, part_rows), jnp.int32),
            pltpu.VMEM((1, part_rows), F32),
            pltpu.VMEM(part_drag.shape, F32),
            pltpu.VMEM(prior_solid.shape, F32),
            pltpu.VMEM(prior_drag.shape, F32),
            dma((HALO_COPIES,)),
            dma((HALO_COPIES,)),
            dma((2, span_size)),
            dma((2, span_size)),
            dma((2,)),
            dma((6,)),
        ],
        compiler_params=far(1),
        name="collect",
    )(
        part_count,
        *[
            pltpu.with_memory_space_constraint(a, pltpu.HBM)
            for a in (
                part_slab.reshape(1, part_rows), part_cell, part_volume, part_drag,
                prior_solid, prior_drag,
            )
        ],
    )
    recv = recv.reshape(5, lines, cols)
    bins = Bins(layers, width_x, width_y, span_size, lines, cols)
    target = pl.pallas_call(
        functools.partial(deposit_kernel, bins),
        out_shape=jax.ShapeDtypeStruct((4, layers, width_x, width_y), F32),
        in_specs=[VMEM],
        out_specs=VMEM,
        compiler_params=LIMIT,
        name="deposit",
    )(recv)
    whole = pltpu.VMEM((4, total_x, layers, width_y + LANES), F32)
    columns = pltpu.VMEM((4, 2, total_x, layers, LANES), F32)
    slots_of = (span_size, per, cols)
    smooth, early_values = pl.pallas_call(
        functools.partial(sweeps_kernel, bins),
        out_shape=(
            jax.ShapeDtypeStruct(target.shape, F32),
            jax.ShapeDtypeStruct((2, *slots_of), F32),
        ),
        in_specs=[VMEM] * 6,
        out_specs=(VMEM, VMEM),
        scratch_shapes=[whole] * 4
        + [columns] * 2
        + [pltpu.VMEM((4, 2, 2, RIM, layers, LANES), F32)]
        + [pltpu.VMEM((layers, 4 * bins.rows, bins.cols), BF)]
        + [dma((4, 2, HALO_COPIES))] * 2
        + [dma((HALO_COPIES,))] * 2,
        compiler_params=far(0),
        name="sweeps",
    )(prior_solid, prior_drag, prior_rows, prior_cols, target, recv)
    fields, early_tables, late_tables, strays = pl.pallas_call(
        functools.partial(fields_kernel, bins),
        out_shape=(
            jax.ShapeDtypeStruct((4, layers, width_x, width_y), F32),
            jax.ShapeDtypeStruct((layers, 4 * bins.rows, bins.cols), BF),
            jax.ShapeDtypeStruct((layers, 4 * bins.rows, bins.cols), BF),
            jax.ShapeDtypeStruct((4, lines, cols), F32),
        ),
        in_specs=[VMEM] * 2,
        out_specs=(VMEM,) * 4,
        scratch_shapes=[pltpu.VMEM((layers, 8 * bins.rows, bins.cols), BF)],
        compiler_params=LIMIT,
        name="fields",
    )(smooth, recv)
    feedback = pl.pallas_call(
        functools.partial(feedback_kernel, bins, wide),
        out_shape=jax.ShapeDtypeStruct((4, 1, part_rows), F32),
        in_specs=[VMEM] * 6,
        out_specs=VMEM,
        scratch_shapes=[
            pltpu.VMEM((4, *slots_of), F32),
            pltpu.VMEM((4, *slots_of), F32),
            pltpu.VMEM((cols, part_rows), BF),
            dma((2, span_size)),
            dma((2, span_size)),
            dma((2,)),
        ],
        compiler_params=far(2),
        name="feedback",
    )(recv, early_values, early_tables, late_tables, strays.reshape(4, *slots_of), slots)
    return (fields, feedback)


def solution(mesh):
    in_specs = (
        P("depth", "span", None),
        P("depth", "span"),
        P("depth", "span"),
        P(None, "depth", "span"),
        P("depth", "span"),
        P(None, "span", "depth"),
        P(None, None, "span", "depth"),
    )
    out_specs = (P(None, None, "span", "depth"), P(None, "depth", "span"))
    return jax.shard_map(
        on_device, mesh=mesh, in_specs=in_specs, out_specs=out_specs, check_vma=False
    )
```

```python
import functools
import math

import jax
import jax.numpy as jnp
from jax import lax
from jax.experimental import pallas as pl
from jax.experimental.pallas import tpu as pltpu
from jax.sharding import PartitionSpec as P

SWEEPS = 6
NU_WEIGHT = 1.0
PHI_LIMIT = 0.6
BF = jnp.bfloat16
F32 = jnp.float32


def two_parts(value):
    high = value.astype(BF)
    return high, (value - high.astype(F32)).astype(BF)


def nt_dot(left, right):
    return lax.dot_general(left, right, (((1,), (1,)), ((), ())), preferred_element_type=F32)


def hot_at(index, count):
    rows = lax.broadcasted_iota(jnp.int32, (count, index.shape[1]), 0)
    return jnp.where(rows == index, 1.0, 0.0).astype(BF)


def spread(values, row, col, rows, cols):
    mask = hot_at(row, rows)
    parts = [two_parts(v) for v in values]
    left = jnp.concatenate([mask * p[k] for k in range(2) for p in parts], axis=0)
    both = nt_dot(left, hot_at(col, cols))
    n = len(values) * rows
    return both[:n] + both[n:]


class Bins:
    def __init__(self, layers, width_x, width_y, span, lines, cols):
        self.layers, self.span, self.lines, self.line = layers, span, lines, cols
        self.binned = lines == span * layers
        self.cols = min(256, width_y)
        self.parts = width_y // self.cols
        self.rows = width_x * self.parts
        self.width_x, self.width_y = width_x, width_y
        self.log_y, self.log_cols = int(math.log2(width_y)), int(math.log2(self.cols))
        self.log_x = int(math.log2(width_x))

    def place(self, ids):
        y = lax.bitwise_and(ids, self.width_y - 1)
        x = lax.bitwise_and(lax.shift_right_arithmetic(ids, self.log_y), self.width_x - 1)
        row = lax.shift_right_arithmetic(y, self.log_cols) * self.width_x + x
        return self.layer(ids) * self.rows + row, lax.bitwise_and(y, self.cols - 1)

    def layer(self, ids):
        return lax.shift_right_arithmetic(ids, self.log_x + self.log_y)

    def strays(self, ids, line, lane):
        live = ids >= 0
        if not self.binned:
            return live
        own = lax.rem(line, self.layers)
        layer = self.layer(ids)
        beside = jnp.where(lane < self.line // 2, own - 1, own + 1)
        return live & (layer != own) & (layer != beside)

    def any_stray(self, ref):
        ids = ref[0].astype(jnp.int32) - 1
        line, lane = (lax.broadcasted_iota(jnp.int32, ids.shape, axis) for axis in range(2))
        mask = self.strays(ids, line, lane)
        return jnp.max(jnp.where(mask, 1.0, 0.0)) > 0.0

    def group(self, ref, c, g):
        block = ref[c, pl.ds(pl.multiple_of(g * 8, 8), 8), :]
        return jnp.concatenate([block[k : k + 1] for k in range(8)], axis=1)

    def stray_group(self, ref, g):
        ids = self.group(ref, 0, g).astype(jnp.int32) - 1
        lane = lax.broadcasted_iota(jnp.int32, ids.shape, 1)
        shift = int(math.log2(self.line))
        line = g * 8 + lax.shift_right_arithmetic(lane, shift)
        return ids, self.strays(ids, line, lax.bitwise_and(lane, self.line - 1))


def add_sums(bins, out, layer, sums):
    for c in range(out.shape[0]):
        for part in range(bins.parts):
            lanes = slice(part * bins.cols, (part + 1) * bins.cols)
            first = c * bins.rows + part * bins.width_x
            out[c, layer, :, lanes] += sums[first : first + bins.width_x]


def near_sums(bins, recv, owners, out):
    comps, half, rows = out.shape[0], bins.line // 2, bins.rows
    for j in range(bins.layers):

        def flat(c, j=j):
            pieces = [
                recv[c, o, pl.ds(j, 1), h * half : (h + 1) * half] for h in range(2) for o in owners
            ]
            return jnp.concatenate(pieces, axis=1)

        ids = flat(0).astype(jnp.int32) - 1
        place, col = bins.place(ids)
        hot = hot_at(col, bins.cols)
        parts = [two_parts(flat(1 + c)) for c in range(comps)]
        n = ids.shape[1] // 2

        def sums(layer, lanes, place=place, hot=hot, parts=parts):
            mask = hot_at(place[:, lanes] - layer * rows, rows)
            left = [mask * p[k][:, lanes] for k in range(2) for p in parts]
            both = nt_dot(jnp.concatenate(left, axis=0), hot[:, lanes])
            add_sums(bins, out, layer, both[: comps * rows] + both[comps * rows :])

        sums(j, slice(0, 2 * n))
        if j > 0:
            sums(j - 1, slice(0, n))
        if j < bins.layers - 1:
            sums(j + 1, slice(n, 2 * n))


def deposit_kernel(bins, near, recv, out):
    comps, rows, cols = out.shape[0], bins.rows, bins.cols
    out[...] = near[...]

    @pl.when(bins.any_stray(recv))
    def _():
        def line_step(g, carry):
            ids, mask = bins.stray_group(recv, g)
            place, col = bins.place(ids)
            values = [jnp.where(mask, bins.group(recv, 1 + c, g), 0.0) for c in range(comps)]

            def layer_step(layer, inner):
                add_sums(bins, out, layer, spread(values, place - layer * rows, col, rows, cols))
                return inner

            return lax.fori_loop(0, bins.layers, layer_step, carry)

        lax.fori_loop(0, bins.lines // 8, line_step, 0)

    out[0] = jnp.minimum(out[0], PHI_LIMIT)


def fill_table(bins, table, fields):
    comps = len(fields)
    for c, value in enumerate(fields):
        high, low = two_parts(value)
        for part in range(bins.parts):
            lanes = slice(part * bins.cols, (part + 1) * bins.cols)
            first = c * bins.rows + part * bins.width_x
            table[pl.ds(first, bins.width_x)] = high[:, lanes]
            table[pl.ds(comps * bins.rows + first, bins.width_x)] = low[:, lanes]


def fields_of(smooth, layer, comps):
    void = 1.0 - smooth[0, layer]
    return [void if c == 0 else -smooth[c, layer] / void for c in comps]


def near_values(bins, tables, ids_ref, lines, out):
    rows, cols, half = bins.rows, bins.cols, bins.line // 2
    height = tables.shape[1]
    comps = height // (2 * rows)
    for j in lines:
        for h in range(2):
            lanes = slice(h * half, (h + 1) * half)
            ids = [ids_ref[0, pl.ds(o * bins.layers + j, 1), lanes] for o in range(bins.span)]
            ids = jnp.concatenate(ids, axis=1).astype(jnp.int32) - 1
            place, col = bins.place(ids)
            low, high = max(j - 1 + h, 0), min(j + h, bins.layers - 1)
            number = high - low + 1
            table = tables[low : high + 1].reshape(number * height, cols)
            wide = jnp.dot(table, hot_at(col, cols), preferred_element_type=F32)
            row = lax.broadcasted_iota(jnp.int32, (rows, ids.shape[1]), 0)
            here = [row == place - layer * rows for layer in range(low, high + 1)]
            for c in range(comps):
                found = 0.0
                for k in range(number):
                    first = k * height + c * rows
                    second = first + comps * rows
                    value = wide[first : first + rows] + wide[second : second + rows]
                    found = jnp.where(here[k], value, found)
                found = jnp.sum(found, axis=0, keepdims=True)
                for o in range(bins.span):
                    out(c, o, j, lanes, found[:, o * half : (o + 1) * half])


def fields_kernel(bins, smooth, ids_ref, fields, early_tables, late_tables, out, tables):
    comps = smooth.shape[0]
    rows, cols = bins.rows, bins.cols
    early = comps // 2

    def table_step(layer, carry):
        values = fields_of(smooth, layer, range(comps))
        for c in range(comps):
            fields[c, layer] = values[c]
        fill_table(bins, early_tables.at[layer], values[:early])
        fill_table(bins, late_tables.at[layer], values[early:])
        return carry

    lax.fori_loop(0, bins.layers, table_step, 0)
    out[...] = jnp.zeros_like(out)

    @pl.when(bins.any_stray(ids_ref))
    def _():
        def all_step(layer, carry):
            fill_table(bins, tables.at[layer], [fields[c, layer] for c in range(comps)])
            return carry

        lax.fori_loop(0, bins.layers, all_step, 0)

        def line_step(g, carry):
            ids, mask = bins.stray_group(ids_ref, g)
            place, col = bins.place(ids)
            hot = hot_at(col, cols)
            row = lax.broadcasted_iota(jnp.int32, (rows, ids.shape[1]), 0)

            def layer_step(layer, total):
                wide = jnp.dot(tables[layer], hot, preferred_element_type=F32)
                here = (row == place - layer * rows) & mask
                more = []
                for c in range(comps):
                    second = (comps + c) * rows
                    value = wide[c * rows : (c + 1) * rows] + wide[second : second + rows]
                    value = jnp.where(here, value, 0.0)
                    more.append(total[c] + jnp.sum(value, axis=0, keepdims=True))
                return more

            zero = [jnp.zeros(ids.shape, F32)] * comps
            total = lax.fori_loop(0, bins.layers, layer_step, zero)
            n = bins.line
            for c in range(comps):
                block = [total[c][:, k * n : (k + 1) * n] for k in range(8)]
                out[c, pl.ds(pl.multiple_of(g * 8, 8), 8), :] = jnp.concatenate(block, axis=0)
            return carry

        lax.fori_loop(0, bins.lines // 8, line_step, 0)


MESH = pl.DeviceIdType.MESH
RIM = SWEEPS // 2
LANES = 128
BATCH = 2


class Grid:
    def __init__(self):
        self.span, self.depth = lax.axis_index("span"), lax.axis_index("depth")
        self.span_size, self.depth_size = lax.axis_size("span"), lax.axis_size("depth")

    def has(self, dx, dy):
        x, y = self.span + dx, self.depth + dy
        return (x >= 0) & (x < self.span_size) & (y >= 0) & (y < self.depth_size)

    def peer(self, dx, dy):
        return (self.span + dx, self.depth + dy)

    def signal(self, barrier, dx, dy):
        @pl.when(self.has(dx, dy))
        def _():
            pl.semaphore_signal(barrier, inc=1, device_id=self.peer(dx, dy), device_id_type=MESH)

    def around(self, steps):
        return sum(self.has(dx, dy).astype(jnp.int32) for dx, dy in steps)


X_STEPS = ((-1, 0), (1, 0))
Y_STEPS = ((0, -1), (0, 1))


class Halo:
    def __init__(self, grid, rows_out, rows_in, edge, columns, send_sem, recv_sem):
        self.grid = grid
        self.rows_out, self.rows_in, self.edge, self.columns = rows_out, rows_in, edge, columns
        self.send_sem, self.recv_sem = send_sem, recv_sem

    def _copy(self, src, dst, at, step):
        return pltpu.make_async_remote_copy(
            src_ref=src,
            dst_ref=dst,
            send_sem=self.send_sem(at),
            recv_sem=self.recv_sem(at),
            device_id=self.grid.peer(*step),
            device_id_type=MESH,
        )

    def rows(self, side):
        return self._copy(self.rows_out(side), self.rows_in(1 - side), side, X_STEPS[side])

    def cols(self, part, side):
        at = 2 + 2 * part + side
        return self._copy(self.edge(part, side), self.columns(part, 1 - side), at, Y_STEPS[side])

    def _when(self, step, action):
        @pl.when(self.grid.has(*step))
        def _():
            action()

    def start(self):
        for side in range(2):
            self._when(X_STEPS[side], lambda: self.rows(side).start())
        self.start_cols((0,))

    def start_cols(self, parts):
        for part in parts:
            for side in range(2):
                self._when(Y_STEPS[side], lambda: self.cols(part, side).start())

    def rows_arrive(self):
        for side in range(2):
            self._when(X_STEPS[1 - side], lambda: self.rows(side).wait_recv())

    def forward(self):
        self.rows_arrive()
        self.start_cols((1, 2))

    def arrive(self, parts=(0, 1, 2)):
        for part in parts:
            for side in range(2):
                self._when(Y_STEPS[1 - side], lambda: self.cols(part, side).wait_recv())

    def rows_sent(self):
        for side in range(2):
            self._when(X_STEPS[side], lambda: self.rows(side).wait_send())

    def cols_sent(self, parts=(0, 1, 2)):
        for part in parts:
            for side in range(2):
                self._when(Y_STEPS[side], lambda: self.cols(part, side).wait_send())

    def sent(self):
        self.rows_sent()
        self.cols_sent()


HALO_COPIES = 8


def collect_kernel(
    bins, cap, block, wide, layers, shift, count, slab_far, cell_far, volume_far, drag_far, solid_far,
    prior_far, recv, slots, rows_in, cols_in, near_target, packed, rows_out, cols_out,
    slab, cell, volume, drag, solid, prior, halo_send, halo_recv, send_sem, recv_sem, own_sem,
    near_sem,
):
    pairs = (
        (slab_far, slab), (cell_far, cell), (solid_far, solid), (prior_far, prior),
        (volume_far, volume), (drag_far, drag),
    )
    near = [pltpu.make_async_copy(a, b, near_sem.at[k]) for k, (a, b) in enumerate(pairs)]
    for copy in near:
        copy.start()
    grid = Grid()
    span_size = grid.span_size
    values, _, per, cols = recv.shape
    lines = span_size * per
    part_rows = slab.shape[1]
    width_x, width_y = solid.shape[1:]
    comps = 1 + prior.shape[0]

    barrier = pltpu.get_barrier_semaphore()
    for k in range(1, span_size):
        to = lax.rem(grid.span + k, span_size)
        pl.semaphore_signal(barrier, inc=1, device_id=(to, grid.depth), device_id_type=MESH)
    for dx, dy in Y_STEPS:
        grid.signal(barrier, dx, dy)

    keys = layers * span_size
    live_count = count[0, 0]
    many = wide // block

    def lanes_at(first, size):
        return pl.ds(pl.multiple_of(first, size), size)

    def member_of(first):
        lanes = lanes_at(first, block)
        live = first + lax.broadcasted_iota(jnp.int32, (1, block), 1) < live_count
        layer = lax.shift_right_arithmetic(cell[:, lanes], shift)
        key = jnp.where(live, layer * span_size + slab[:, lanes], -1)
        member = jnp.where(lax.broadcasted_iota(jnp.int32, (keys, block), 0) == key, 1.0, 0.0)
        return member, live

    fold = min(block, LANES)

    def tally(b, total):
        for m in range(many):
            member = member_of(b * wide + m * block)[0]
            for k in range(block // fold):
                total = total + member[:, k * fold : (k + 1) * fold]
        return total

    near[0].wait()
    near[1].wait()
    total = lax.fori_loop(0, part_rows // wide, tally, jnp.zeros((keys, fold), F32))
    near[2].wait()
    near[3].wait()
    for c in range(comps):
        field = solid if c == 0 else prior.at[c - 1]
        for x in range(width_x):
            line = field[:, x, :]
            if x < RIM:
                rows_out[c, 0, x] = line
            if x >= width_x - RIM:
                rows_out[c, 1, x - width_x + RIM] = line
            cols_out[c, 0, x] = line[:, :LANES]
            cols_out[c, 1, x] = line[:, width_y - LANES :]
    for side in range(2):

        @pl.when(jnp.logical_not(grid.has(*X_STEPS[side])))
        def _(side=side):
            rows_in[:, side] = jnp.zeros((comps, RIM, layers, width_y), F32)

        @pl.when(jnp.logical_not(grid.has(*Y_STEPS[side])))
        def _(side=side):
            cols_in[:, side] = jnp.zeros((comps, width_x, layers, LANES), F32)

    def halo_of(at):
        mine = pl.ds(*((0, comps // 2), (comps // 2, comps - comps // 2))[at])
        return Halo(
            grid,
            lambda side: rows_out.at[mine, side],
            lambda side: rows_in.at[mine, side],
            lambda part, side: cols_out.at[mine, side],
            lambda part, side: cols_in.at[mine, side],
            lambda copy: halo_send.at[at, copy],
            lambda copy: halo_recv.at[at, copy],
        )

    halos = [halo_of(at) for at in range(2)]
    pl.semaphore_wait(barrier, span_size - 1 + grid.around(Y_STEPS))
    halos[0].start()

    before_lane = lax.broadcasted_iota(jnp.int32, (block, block), 0)
    this_lane = lax.broadcasted_iota(jnp.int32, (block, block), 1)
    tri = jnp.where(before_lane < this_lane, 1.0, 0.0).astype(BF)
    total = jnp.sum(total, axis=1, keepdims=True)
    counts = [total[k * span_size : (k + 1) * span_size] for k in range(layers)]
    rest = [None] * layers
    left = jnp.zeros((span_size, 1), F32)
    for k in reversed(range(layers)):
        left = left + counts[k]
        rest[k] = left
    base = lax.broadcasted_iota(jnp.int32, (span_size, 1), 0).astype(F32) * cap
    end = jnp.zeros((span_size, 1), F32)
    starts = []
    for k in range(layers):
        start = jnp.minimum(jnp.maximum(end, float(cap // layers * k)), cap - rest[k])
        starts.append(start + base)
        end = start + counts[k]

    def rank(b, offset):
        for m in range(many):
            first = b * wide + m * block
            member, live = member_of(first)
            before = jnp.dot(member.astype(BF), tri, preferred_element_type=F32)
            place = jnp.sum(member * (before + offset), axis=0, keepdims=True).astype(jnp.int32)
            slots[:, lanes_at(first, block)] = jnp.where(live, place, -1)
            offset = offset + jnp.sum(member, axis=1, keepdims=True)
        return offset

    lax.fori_loop(0, part_rows // wide, rank, jnp.concatenate(starts, axis=0))

    near[4].wait()
    near[5].wait()
    groups = ((0, 2), (2, values - 2))

    def own_copy(at):
        mine = pl.ds(*groups[at])
        return pltpu.make_async_copy(
            packed.at[mine, grid.span], recv.at[mine, grid.span], own_sem.at[at]
        )

    def copy_to(at, k):
        mine = pl.ds(*groups[at])
        to = lax.rem(grid.span + k, span_size)
        return pltpu.make_async_remote_copy(
            src_ref=packed.at[mine, to],
            dst_ref=recv.at[mine, grid.span],
            send_sem=send_sem.at[at, k],
            recv_sem=recv_sem.at[at, k],
            device_id=(to, grid.depth),
            device_id_type=MESH,
        )

    for at, (first_value, number) in enumerate(groups):
        mine = pl.ds(first_value, number)

        def place_values(b, carry, first_value=first_value, number=number, mine=mine):
            lanes = lanes_at(b * wide, wide)
            slot = slots[:, lanes]
            row = lax.shift_right_arithmetic(slot, int(math.log2(cols)))
            col = lax.bitwise_and(slot, cols - 1)
            taken = []
            for v in range(first_value, first_value + number):
                if v == 0:
                    taken.append((cell[:, lanes] + 1).astype(F32))
                else:
                    taken.append(volume[:, lanes] if v == 1 else drag[v - 2, :, lanes])
            sums = spread(taken, row, col, lines, cols).reshape(number, span_size, per, cols)
            packed[mine] += sums
            return carry

        packed[mine] = jnp.zeros((number, span_size, per, cols), F32)
        lax.fori_loop(0, part_rows // wide, place_values, 0)
        own_copy(at).start()
        for k in range(1, span_size):
            copy_to(at, k).start()
    halos[1].start()
    near_target[...] = jnp.zeros_like(near_target)
    for at in range(len(groups)):
        own_copy(at).wait()
    if bins.binned:
        batch = math.gcd(span_size, BATCH)

        def batch_step(b, carry):
            owners = []
            for i in range(batch):
                k = b * batch + i

                @pl.when(k > 0)
                def _(k=k):
                    for at in range(len(groups)):
                        copy_to(at, k).wait_recv()

                owners.append(lax.rem(grid.span + span_size - k, span_size))
            near_sums(bins, recv, owners, near_target)
            return carry

        lax.fori_loop(0, span_size // batch, batch_step, 0)
    else:
        for at in range(len(groups)):
            for k in range(1, span_size):
                copy_to(at, k).wait_recv()
    for at in range(len(groups)):
        for k in range(1, span_size):
            copy_to(at, k).wait_send()
    for halo in halos:
        halo.rows_arrive()
        halo.arrive((0,))
        halo.rows_sent()
        halo.cols_sent((0,))


def sweeps_kernel(
    bins, solid_far, prior_far, prior_rows, prior_cols, target, ids_ref, out, early_values,
    solid, prior, near_sem, source, first, second, middle, source_cols, middle_cols, corners, tables, send_sem, recv_sem,
    corner_send, corner_recv,
):
    grid = Grid()
    comps, layers, width_x, width_y = target.shape
    near = [
        pltpu.make_async_copy(a, b, near_sem.at[k])
        for k, (a, b) in enumerate(((solid_far, solid), (prior_far, prior)))
    ]
    for copy in near:
        copy.start()
    total_x = width_x + 2 * RIM
    own = pl.ds(0, width_y)
    rest = pl.ds(width_y, LANES)
    own_rows = pl.ds(RIM, width_x)

    barrier = pltpu.get_barrier_semaphore()
    for dx, dy in X_STEPS + Y_STEPS:
        grid.signal(barrier, dx, dy)

    def halo_of(c, phase):
        buffer, cols_in = (source, source_cols) if phase == 0 else (middle, middle_cols)
        width = RIM - 1 if phase == 0 else RIM

        def rows_out(side):
            return buffer.at[c, pl.ds(RIM if side == 0 else RIM + width_x - width, width), :, own]

        def rows_in(side):
            return buffer.at[c, pl.ds(RIM - width if side == 0 else RIM + width_x, width), :, own]

        def rows_of(part):
            return pl.ds(*((RIM, width_x), (RIM - width, width), (RIM + width_x, width))[part])

        def edge(part, side):
            lanes = pl.ds(0 if side == 0 else width_y - LANES, LANES)
            return buffer.at[c, rows_of(part), :, lanes]

        def columns(part, side):
            return cols_in.at[c, side, rows_of(part)]

        return Halo(
            grid, rows_out, rows_in, edge, columns,
            lambda at: send_sem.at[c, phase, at], lambda at: recv_sem.at[c, phase, at],
        )

    def corner_edge(part, side):
        lanes = pl.ds(0 if side == 0 else width_y - LANES, LANES)
        return prior_rows.at[:, part - 1, :, :, lanes]

    around = Halo(
        grid, None, None, corner_edge, lambda part, side: corners.at[:, side, part - 1],
        lambda at: corner_send.at[at], lambda at: corner_recv.at[at],
    )
    halos = [[halo_of(c, phase) for phase in range(2)] for c in range(comps)]
    lane = lax.broadcasted_iota(jnp.int32, (1, layers, LANES), 2)

    def fill_cols(buffer, c, cols_in):
        buffer[c, :, :, rest] = jnp.where(lane < LANES // 2, cols_in[c, 1], cols_in[c, 0])

    for c in range(comps):
        for x in range(width_x):
            source[c, RIM + x, :, own] = target[c, :, x, :]
    for copy in near:
        copy.wait()
    for c in range(comps):
        field = solid if c == 0 else prior.at[c - 1]
        for x in range(width_x):
            first[c, RIM + x, :, own] = field[:, x, :]
        first[c, pl.ds(0, RIM), :, own] = prior_rows[c, 0]
        first[c, pl.ds(RIM + width_x, RIM), :, own] = prior_rows[c, 1]
        first[c, own_rows, :, rest] = jnp.where(lane < LANES // 2, prior_cols[c, 1], prior_cols[c, 0])

    pl.semaphore_wait(barrier, grid.around(X_STEPS + Y_STEPS))
    for c in range(comps):
        halos[c][0].start()
    around.start_cols((1, 2))
    for side, at in ((0, 0), (1, RIM + width_x)):

        @pl.when(jnp.logical_not(grid.has(*X_STEPS[side])))
        def _(at=at):
            for buffer in (source, middle):
                zeros = jnp.zeros((comps, RIM, layers, width_y), F32)
                buffer[:, pl.ds(at, RIM), :, own] = zeros

        @pl.when(jnp.logical_not(grid.has(*Y_STEPS[side])))
        def _(side=side):
            for buffer in (source_cols, middle_cols):
                buffer[:, side] = jnp.zeros((comps, total_x, layers, LANES), F32)
            corners[:, side] = jnp.zeros((comps, 2, RIM, layers, LANES), F32)

    lanes = lax.broadcasted_iota(jnp.int32, (layers, width_y + LANES), 1)
    known = lanes < width_y
    known = known | ((lanes < width_y + LANES // 2) & (grid.depth < grid.depth_size - 1))
    known = known | ((lanes >= width_y + LANES // 2) & (grid.depth > 0))
    scale = jnp.where(known, 1.0 / (1.0 + 4.0 * NU_WEIGHT), 0.0)

    def relax(c, x, before, here, after):
        beside = before + after
        beside = beside + pltpu.roll(here, 1, 1) + pltpu.roll(here, width_y + LANES - 1, 1)
        return (source[c, x] + NU_WEIGHT * beside) * scale

    def sweep(c, old, new, gone):
        low, high = gone, total_x - gone
        step = max(k for k in range(1, 9) if (high - low) % k == 0)

        def rows(g, carry):
            before, here = carry
            for k in range(step):
                x = low + g * step + k
                after = old[c, x + 1]
                new[c, x] = relax(c, x, before, here, after)
                before, here = here, after
            return before, here

        lax.fori_loop(0, (high - low) // step, rows, (old[c, low - 1], old[c, low]))
        for side, x in ((0, RIM - 1), (1, RIM + width_x)):
            if low <= x < high:

                @pl.when(jnp.logical_not(grid.has(*X_STEPS[side])))
                def _(x=x):
                    new[c, x] = jnp.zeros((layers, width_y + LANES), F32)

    def first_half(c):
        halos[c][0].arrive()
        fill_cols(source, c, source_cols)
        sweep(c, first, second, 1)
        sweep(c, second, first, 2)
        sweep(c, first, middle, 3)
        halos[c][1].start()

    def second_half(c):
        halos[c][1].arrive()
        fill_cols(middle, c, middle_cols)
        sweep(c, middle, first, 1)
        sweep(c, first, second, 2)
        before, here = second[c, RIM - 1], second[c, RIM]
        for x in range(width_x):
            after = second[c, RIM + x + 1]
            out[c, :, x, :] = relax(c, RIM + x, before, here, after)[:, :width_y]
            before, here = here, after

    around.arrive((1, 2))
    for c in range(comps):
        for part, at in ((0, 0), (1, RIM + width_x)):
            first[c, pl.ds(at, RIM), :, rest] = jnp.where(
                lane < LANES // 2, corners[c, 1, part], corners[c, 0, part]
            )
    halos[0][0].forward()
    for c in range(comps):
        if c + 1 < comps:
            halos[c + 1][0].forward()
        first_half(c)
    early = early_values.shape[0]
    parts = comps - early

    early_values[...] = jnp.zeros_like(early_values)

    def put(c, owner, line, lanes, value):
        early_values[c, owner, pl.ds(line, 1), lanes] = value

    halos[0][1].forward()
    for c in range(comps):
        if c + 1 < comps:
            halos[c + 1][1].forward()
        second_half(c)
        if not bins.binned:
            continue
        if c == early - 1:

            def table_step(layer, carry):
                fill_table(bins, tables.at[layer], fields_of(out, layer, range(early)))
                return carry

            lax.fori_loop(0, layers, table_step, 0)
        if early - 1 <= c < comps - 1:
            at = c - early + 1
            share = layers // (2 * parts)
            lines = range(share * at, share * (at + 1))
            near_values(bins, tables, ids_ref, lines, put)
    for c in range(comps):
        for phase in range(2):
            halos[c][phase].sent()
    around.cols_sent((1, 2))


def feedback_kernel(
    bins, wide, ids_ref, early_values, early_tables, late_tables, strays, slots, out,
    values, table, hots, send_sem, recv_sem, own_sem,
):
    grid = Grid()
    comps, span_size, per, cols = values.shape
    lines = span_size * per
    part_rows = slots.shape[1]
    early = early_values.shape[0]
    barrier = pltpu.get_barrier_semaphore()
    for k in range(1, span_size):
        to = lax.rem(grid.span + k, span_size)
        pl.semaphore_signal(barrier, inc=1, device_id=(to, grid.depth), device_id_type=MESH)

    def put(c, owner, line, lanes, value):
        more = strays[early + c, owner, pl.ds(line, 1), lanes]
        values[early + c, owner, pl.ds(line, 1), lanes] = value + more

    def put_early(c, owner, line, lanes, value):
        more = strays[c, owner, pl.ds(line, 1), lanes]
        values[c, owner, pl.ds(line, 1), lanes] = value + more

    values[pl.ds(0, early)] = early_values[...] + strays[pl.ds(0, early)]
    copies = []

    def send(first, number):
        mine = pl.ds(first, number)
        at = len(copies)
        started = [
            pltpu.make_async_copy(
                values.at[mine, grid.span], table.at[mine, grid.span], own_sem.at[at]
            )
        ]
        for k in range(1, span_size):
            to = lax.rem(grid.span + k, span_size)
            started.append(
                pltpu.make_async_remote_copy(
                    src_ref=values.at[mine, to],
                    dst_ref=table.at[mine, grid.span],
                    send_sem=send_sem.at[at, k],
                    recv_sem=recv_sem.at[at, k],
                    device_id=(to, grid.depth),
                    device_id_type=MESH,
                )
            )
        for copy in started:
            copy.start()
        copies.append((mine, started))

    half = bins.layers // 2
    if bins.binned:
        near_values(bins, early_tables, ids_ref, range(half, bins.layers), put_early)
    else:
        values[pl.ds(early, comps - early)] = strays[pl.ds(early, comps - early)]
    pl.semaphore_wait(barrier, span_size - 1)
    send(0, early)
    if bins.binned:
        near_values(bins, late_tables, ids_ref, range(bins.layers), put)
    send(early, comps - early)

    def lanes_at(b):
        return pl.ds(pl.multiple_of(b * wide, wide), wide)

    def hot_step(b, carry):
        lanes = lanes_at(b)
        hots[:, lanes] = hot_at(lax.bitwise_and(slots[:, lanes], cols - 1), cols)
        return carry

    lax.fori_loop(0, part_rows // wide, hot_step, 0)
    for mine, started in copies:
        for copy in started:
            copy.wait()
        number = mine.size
        high, low = two_parts(table[mine].reshape(number * lines, cols))
        both = jnp.concatenate([high, low], axis=0)

        def pick_step(b, carry, mine=mine, number=number, both=both):
            lanes = lanes_at(b)
            row = lax.shift_right_arithmetic(slots[:, lanes], int(math.log2(cols)))
            wanted = lax.broadcasted_iota(jnp.int32, (lines, wide), 0) == row
            found = jnp.dot(both, hots[:, lanes], preferred_element_type=F32)
            for c in range(number):
                value = found[c * lines : (c + 1) * lines]
                value = value + found[(number + c) * lines : (number + c + 1) * lines]
                value = jnp.sum(jnp.where(wanted, value, 0.0), axis=0, keepdims=True)
                out[mine.start + c, :, lanes] = value
            return carry

        lax.fori_loop(0, part_rows // wide, pick_step, 0)


VMEM = pl.BlockSpec(memory_space=pltpu.VMEM)
SMEM = pl.BlockSpec(memory_space=pltpu.SMEM)
HBM = pl.BlockSpec(memory_space=pltpu.HBM)
LIMIT = pltpu.CompilerParams(vmem_limit_bytes=48 * 1024 * 1024)


def far(number):
    return pltpu.CompilerParams(
        vmem_limit_bytes=48 * 1024 * 1024, collective_id=number, has_side_effects=True
    )


def on_device(part_slab, part_cell, part_volume, part_drag, part_count, prior_solid, prior_drag):
    span_size = lax.axis_size("span")
    part_rows = part_cell.shape[1]
    cap = 2 * part_rows // span_size
    layers, width_x, width_y = prior_solid.shape
    cols = min(256, cap)
    lines = span_size * cap // cols
    per = lines // span_size
    block = math.gcd(part_rows, 512)
    wide = math.gcd(part_rows, 2048)
    total_x = width_x + 2 * RIM
    dma = pltpu.SemaphoreType.DMA
    bins = Bins(layers, width_x, width_y, span_size, lines, cols)
    recv, slots, prior_rows, prior_cols, near_target = pl.pallas_call(
        functools.partial(
            collect_kernel, bins, cap, block, wide, layers, int(math.log2(width_x * width_y))
        ),
        out_shape=(
            jax.ShapeDtypeStruct((5, span_size, per, cols), F32),
            jax.ShapeDtypeStruct((1, part_rows), jnp.int32),
            jax.ShapeDtypeStruct((4, 2, RIM, layers, width_y), F32),
            jax.ShapeDtypeStruct((4, 2, width_x, layers, LANES), F32),
            jax.ShapeDtypeStruct((4, layers, width_x, width_y), F32),
        ),
        in_specs=[SMEM] + [HBM] * 6,
        out_specs=(VMEM,) * 5,
        scratch_shapes=[
            pltpu.VMEM((5, span_size, per, cols), F32),
            pltpu.VMEM((4, 2, RIM, layers, width_y), F32),
            pltpu.VMEM((4, 2, width_x, layers, LANES), F32),
            pltpu.VMEM((1, part_rows), jnp.int32),
            pltpu.VMEM((1, part_rows), jnp.int32),
            pltpu.VMEM((1, part_rows), F32),
            pltpu.VMEM(part_drag.shape, F32),
            pltpu.VMEM(prior_solid.shape, F32),
            pltpu.VMEM(prior_drag.shape, F32),
            dma((2, HALO_COPIES)),
            dma((2, HALO_COPIES)),
            dma((2, span_size)),
            dma((2, span_size)),
            dma((2,)),
            dma((6,)),
        ],
        compiler_params=far(1),
        name="collect",
    )(
        part_count,
        *[
            pltpu.with_memory_space_constraint(a, pltpu.HBM)
            for a in (
                part_slab.reshape(1, part_rows), part_cell, part_volume, part_drag,
                prior_solid, prior_drag,
            )
        ],
    )
    recv = recv.reshape(5, lines, cols)
    target = pl.pallas_call(
        functools.partial(deposit_kernel, bins),
        out_shape=jax.ShapeDtypeStruct((4, layers, width_x, width_y), F32),
        in_specs=[VMEM] * 2,
        out_specs=VMEM,
        compiler_params=LIMIT,
        name="deposit",
    )(near_target, recv)
    whole = pltpu.VMEM((4, total_x, layers, width_y + LANES), F32)
    columns = pltpu.VMEM((4, 2, total_x, layers, LANES), F32)
    slots_of = (span_size, per, cols)
    smooth, early_values = pl.pallas_call(
        functools.partial(sweeps_kernel, bins),
        out_shape=(
            jax.ShapeDtypeStruct(target.shape, F32),
            jax.ShapeDtypeStruct((2, *slots_of), F32),
        ),
        in_specs=[HBM] * 2 + [VMEM] * 4,
        out_specs=(VMEM, VMEM),
        scratch_shapes=[
            pltpu.VMEM(prior_solid.shape, F32),
            pltpu.VMEM(prior_drag.shape, F32),
            dma((2,)),
        ]
        + [whole] * 4
        + [columns] * 2
        + [pltpu.VMEM((4, 2, 2, RIM, layers, LANES), F32)]
        + [pltpu.VMEM((layers, 4 * bins.rows, bins.cols), BF)]
        + [dma((4, 2, HALO_COPIES))] * 2
        + [dma((HALO_COPIES,))] * 2,
        compiler_params=far(0),
        name="sweeps",
    )(
        pltpu.with_memory_space_constraint(prior_solid, pltpu.HBM),
        pltpu.with_memory_space_constraint(prior_drag, pltpu.HBM),
        prior_rows, prior_cols, target, recv,
    )
    fields, early_tables, late_tables, strays = pl.pallas_call(
        functools.partial(fields_kernel, bins),
        out_shape=(
            jax.ShapeDtypeStruct((4, layers, width_x, width_y), F32),
            jax.ShapeDtypeStruct((layers, 4 * bins.rows, bins.cols), BF),
            jax.ShapeDtypeStruct((layers, 4 * bins.rows, bins.cols), BF),
            jax.ShapeDtypeStruct((4, lines, cols), F32),
        ),
        in_specs=[VMEM] * 2,
        out_specs=(VMEM,) * 4,
        scratch_shapes=[pltpu.VMEM((layers, 8 * bins.rows, bins.cols), BF)],
        compiler_params=LIMIT,
        name="fields",
    )(smooth, recv)
    feedback = pl.pallas_call(
        functools.partial(feedback_kernel, bins, wide),
        out_shape=jax.ShapeDtypeStruct((4, 1, part_rows), F32),
        in_specs=[VMEM] * 6,
        out_specs=VMEM,
        scratch_shapes=[
            pltpu.VMEM((4, *slots_of), F32),
            pltpu.VMEM((4, *slots_of), F32),
            pltpu.VMEM((cols, part_rows), BF),
            dma((2, span_size)),
            dma((2, span_size)),
            dma((2,)),
        ],
        compiler_params=far(2),
        name="feedback",
    )(recv, early_values, early_tables, late_tables, strays.reshape(4, *slots_of), slots)
    return (fields, feedback)


def solution(mesh):
    in_specs = (
        P("depth", "span", None),
        P("depth", "span"),
        P("depth", "span"),
        P(None, "depth", "span"),
        P("depth", "span"),
        P(None, "span", "depth"),
        P(None, None, "span", "depth"),
    )
    out_specs = (P(None, None, "span", "depth"), P(None, "depth", "span"))
    return jax.shard_map(
        on_device, mesh=mesh, in_specs=in_specs, out_specs=out_specs, check_vma=False
    )
```

```python
import functools
import math

import jax
import jax.numpy as jnp
from jax import lax
from jax.experimental import pallas as pl
from jax.experimental.pallas import tpu as pltpu
from jax.sharding import PartitionSpec as P

SWEEPS = 6
NU_WEIGHT = 1.0
PHI_LIMIT = 0.6
BF = jnp.bfloat16
F32 = jnp.float32


def two_parts(value):
    high = value.astype(BF)
    return high, (value - high.astype(F32)).astype(BF)


def nt_dot(left, right):
    return lax.dot_general(left, right, (((1,), (1,)), ((), ())), preferred_element_type=F32)


def hot_at(index, count):
    rows = lax.broadcasted_iota(jnp.int32, (count, index.shape[1]), 0)
    return jnp.where(rows == index, 1.0, 0.0).astype(BF)


def spread(values, row, col, rows, cols):
    mask = hot_at(row, rows)
    parts = [two_parts(v) for v in values]
    left = jnp.concatenate([mask * p[k] for k in range(2) for p in parts], axis=0)
    both = nt_dot(left, hot_at(col, cols))
    n = len(values) * rows
    return both[:n] + both[n:]


class Bins:
    def __init__(self, layers, width_x, width_y, span, lines, cols):
        self.layers, self.span, self.lines, self.line = layers, span, lines, cols
        self.binned = lines == span * layers
        self.cols = min(256, width_y)
        self.parts = width_y // self.cols
        self.rows = width_x * self.parts
        self.width_x, self.width_y = width_x, width_y
        self.log_y, self.log_cols = int(math.log2(width_y)), int(math.log2(self.cols))
        self.log_x = int(math.log2(width_x))

    def place(self, ids):
        y = lax.bitwise_and(ids, self.width_y - 1)
        x = lax.bitwise_and(lax.shift_right_arithmetic(ids, self.log_y), self.width_x - 1)
        row = lax.shift_right_arithmetic(y, self.log_cols) * self.width_x + x
        return self.layer(ids) * self.rows + row, lax.bitwise_and(y, self.cols - 1)

    def layer(self, ids):
        return lax.shift_right_arithmetic(ids, self.log_x + self.log_y)

    def strays(self, ids, line, lane):
        live = ids >= 0
        if not self.binned:
            return live
        own = lax.rem(line, self.layers)
        layer = self.layer(ids)
        beside = jnp.where(lane < self.line // 2, own - 1, own + 1)
        return live & (layer != own) & (layer != beside)

    def any_stray(self, ref):
        ids = ref[0].astype(jnp.int32) - 1
        line, lane = (lax.broadcasted_iota(jnp.int32, ids.shape, axis) for axis in range(2))
        mask = self.strays(ids, line, lane)
        return jnp.max(jnp.where(mask, 1.0, 0.0)) > 0.0

    def group(self, ref, c, g):
        block = ref[c, pl.ds(pl.multiple_of(g * 8, 8), 8), :]
        return jnp.concatenate([block[k : k + 1] for k in range(8)], axis=1)

    def stray_group(self, ref, g):
        ids = self.group(ref, 0, g).astype(jnp.int32) - 1
        lane = lax.broadcasted_iota(jnp.int32, ids.shape, 1)
        shift = int(math.log2(self.line))
        line = g * 8 + lax.shift_right_arithmetic(lane, shift)
        return ids, self.strays(ids, line, lax.bitwise_and(lane, self.line - 1))


def add_sums(bins, out, layer, sums):
    for c in range(out.shape[0]):
        for part in range(bins.parts):
            lanes = slice(part * bins.cols, (part + 1) * bins.cols)
            first = c * bins.rows + part * bins.width_x
            out[c, layer, :, lanes] += sums[first : first + bins.width_x]


def near_sums(bins, recv, owners, out):
    comps, half, rows = out.shape[0], bins.line // 2, bins.rows
    for j in range(bins.layers):

        def flat(c, j=j):
            pieces = [
                recv[c, o, pl.ds(j, 1), h * half : (h + 1) * half] for h in range(2) for o in owners
            ]
            return jnp.concatenate(pieces, axis=1)

        ids = flat(0).astype(jnp.int32) - 1
        place, col = bins.place(ids)
        hot = hot_at(col, bins.cols)
        parts = [two_parts(flat(1 + c)) for c in range(comps)]
        n = ids.shape[1] // 2

        def sums(layer, lanes, place=place, hot=hot, parts=parts):
            mask = hot_at(place[:, lanes] - layer * rows, rows)
            left = [mask * p[k][:, lanes] for k in range(2) for p in parts]
            both = nt_dot(jnp.concatenate(left, axis=0), hot[:, lanes])
            add_sums(bins, out, layer, both[: comps * rows] + both[comps * rows :])

        sums(j, slice(0, 2 * n))
        if j > 0:
            sums(j - 1, slice(0, n))
        if j < bins.layers - 1:
            sums(j + 1, slice(n, 2 * n))


def deposit_kernel(bins, near, recv, out):
    comps, rows, cols = out.shape[0], bins.rows, bins.cols
    out[...] = near[...]

    @pl.when(bins.any_stray(recv))
    def _():
        def line_step(g, carry):
            ids, mask = bins.stray_group(recv, g)
            place, col = bins.place(ids)
            values = [jnp.where(mask, bins.group(recv, 1 + c, g), 0.0) for c in range(comps)]

            def layer_step(layer, inner):
                add_sums(bins, out, layer, spread(values, place - layer * rows, col, rows, cols))
                return inner

            return lax.fori_loop(0, bins.layers, layer_step, carry)

        lax.fori_loop(0, bins.lines // 8, line_step, 0)

    out[0] = jnp.minimum(out[0], PHI_LIMIT)


def fill_table(bins, table, fields):
    comps = len(fields)
    for c, value in enumerate(fields):
        high, low = two_parts(value)
        for part in range(bins.parts):
            lanes = slice(part * bins.cols, (part + 1) * bins.cols)
            first = c * bins.rows + part * bins.width_x
            table[pl.ds(first, bins.width_x)] = high[:, lanes]
            table[pl.ds(comps * bins.rows + first, bins.width_x)] = low[:, lanes]


def fields_of(smooth, layer, comps):
    void = 1.0 - smooth[0, layer]
    return [void if c == 0 else -smooth[c, layer] / void for c in comps]


def near_values(bins, tables, ids_ref, lines, out):
    rows, cols, half = bins.rows, bins.cols, bins.line // 2
    height = tables.shape[1]
    comps = height // (2 * rows)
    for j in lines:
        for h in range(2):
            lanes = slice(h * half, (h + 1) * half)
            ids = [ids_ref[0, pl.ds(o * bins.layers + j, 1), lanes] for o in range(bins.span)]
            ids = jnp.concatenate(ids, axis=1).astype(jnp.int32) - 1
            place, col = bins.place(ids)
            low, high = max(j - 1 + h, 0), min(j + h, bins.layers - 1)
            number = high - low + 1
            table = tables[low : high + 1].reshape(number * height, cols)
            wide = jnp.dot(table, hot_at(col, cols), preferred_element_type=F32)
            row = lax.broadcasted_iota(jnp.int32, (rows, ids.shape[1]), 0)
            here = [row == place - layer * rows for layer in range(low, high + 1)]
            for c in range(comps):
                found = 0.0
                for k in range(number):
                    first = k * height + c * rows
                    second = first + comps * rows
                    value = wide[first : first + rows] + wide[second : second + rows]
                    found = jnp.where(here[k], value, found)
                found = jnp.sum(found, axis=0, keepdims=True)
                for o in range(bins.span):
                    out(c, o, j, lanes, found[:, o * half : (o + 1) * half])


def fields_kernel(bins, smooth, ids_ref, fields, early_tables, late_tables, out, tables):
    comps = smooth.shape[0]
    rows, cols = bins.rows, bins.cols
    early = comps // 2

    def table_step(layer, carry):
        values = fields_of(smooth, layer, range(comps))
        for c in range(comps):
            fields[c, layer] = values[c]
        fill_table(bins, early_tables.at[layer], values[:early])
        fill_table(bins, late_tables.at[layer], values[early:])
        return carry

    lax.fori_loop(0, bins.layers, table_step, 0)
    out[...] = jnp.zeros_like(out)

    @pl.when(bins.any_stray(ids_ref))
    def _():
        def all_step(layer, carry):
            fill_table(bins, tables.at[layer], [fields[c, layer] for c in range(comps)])
            return carry

        lax.fori_loop(0, bins.layers, all_step, 0)

        def line_step(g, carry):
            ids, mask = bins.stray_group(ids_ref, g)
            place, col = bins.place(ids)
            hot = hot_at(col, cols)
            row = lax.broadcasted_iota(jnp.int32, (rows, ids.shape[1]), 0)

            def layer_step(layer, total):
                wide = jnp.dot(tables[layer], hot, preferred_element_type=F32)
                here = (row == place - layer * rows) & mask
                more = []
                for c in range(comps):
                    second = (comps + c) * rows
                    value = wide[c * rows : (c + 1) * rows] + wide[second : second + rows]
                    value = jnp.where(here, value, 0.0)
                    more.append(total[c] + jnp.sum(value, axis=0, keepdims=True))
                return more

            zero = [jnp.zeros(ids.shape, F32)] * comps
            total = lax.fori_loop(0, bins.layers, layer_step, zero)
            n = bins.line
            for c in range(comps):
                block = [total[c][:, k * n : (k + 1) * n] for k in range(8)]
                out[c, pl.ds(pl.multiple_of(g * 8, 8), 8), :] = jnp.concatenate(block, axis=0)
            return carry

        lax.fori_loop(0, bins.lines // 8, line_step, 0)


MESH = pl.DeviceIdType.MESH
RIM = SWEEPS // 2
LANES = 128
BATCH = 2


class Grid:
    def __init__(self):
        self.span, self.depth = lax.axis_index("span"), lax.axis_index("depth")
        self.span_size, self.depth_size = lax.axis_size("span"), lax.axis_size("depth")

    def has(self, dx, dy):
        x, y = self.span + dx, self.depth + dy
        return (x >= 0) & (x < self.span_size) & (y >= 0) & (y < self.depth_size)

    def peer(self, dx, dy):
        return (self.span + dx, self.depth + dy)

    def signal(self, barrier, dx, dy):
        @pl.when(self.has(dx, dy))
        def _():
            pl.semaphore_signal(barrier, inc=1, device_id=self.peer(dx, dy), device_id_type=MESH)

    def around(self, steps):
        return sum(self.has(dx, dy).astype(jnp.int32) for dx, dy in steps)


X_STEPS = ((-1, 0), (1, 0))
Y_STEPS = ((0, -1), (0, 1))


class Halo:
    def __init__(self, grid, rows_out, rows_in, edge, columns, send_sem, recv_sem):
        self.grid = grid
        self.rows_out, self.rows_in, self.edge, self.columns = rows_out, rows_in, edge, columns
        self.send_sem, self.recv_sem = send_sem, recv_sem

    def _copy(self, src, dst, at, step):
        return pltpu.make_async_remote_copy(
            src_ref=src,
            dst_ref=dst,
            send_sem=self.send_sem(at),
            recv_sem=self.recv_sem(at),
            device_id=self.grid.peer(*step),
            device_id_type=MESH,
        )

    def rows(self, side):
        return self._copy(self.rows_out(side), self.rows_in(1 - side), side, X_STEPS[side])

    def cols(self, part, side):
        at = 2 + 2 * part + side
        return self._copy(self.edge(part, side), self.columns(part, 1 - side), at, Y_STEPS[side])

    def _when(self, step, action):
        @pl.when(self.grid.has(*step))
        def _():
            action()

    def start(self):
        for side in range(2):
            self._when(X_STEPS[side], lambda: self.rows(side).start())
        self.start_cols((0,))

    def start_cols(self, parts):
        for part in parts:
            for side in range(2):
                self._when(Y_STEPS[side], lambda: self.cols(part, side).start())

    def rows_arrive(self):
        for side in range(2):
            self._when(X_STEPS[1 - side], lambda: self.rows(side).wait_recv())

    def forward(self):
        self.rows_arrive()
        self.start_cols((1, 2))

    def arrive(self, parts=(0, 1, 2)):
        for part in parts:
            for side in range(2):
                self._when(Y_STEPS[1 - side], lambda: self.cols(part, side).wait_recv())

    def rows_sent(self):
        for side in range(2):
            self._when(X_STEPS[side], lambda: self.rows(side).wait_send())

    def cols_sent(self, parts=(0, 1, 2)):
        for part in parts:
            for side in range(2):
                self._when(Y_STEPS[side], lambda: self.cols(part, side).wait_send())

    def sent(self):
        self.rows_sent()
        self.cols_sent()


HALO_COPIES = 8


def collect_kernel(
    bins, cap, block, wide, layers, shift, count, slab_far, cell_far, volume_far, drag_far, solid_far,
    prior_far, recv, slots, rows_in, cols_in, near_target, packed, rows_out, cols_out,
    slab, cell, volume, drag, solid, prior, halo_send, halo_recv, send_sem, recv_sem, own_sem,
    near_sem,
):
    pairs = (
        (slab_far, slab), (cell_far, cell), (solid_far, solid), (prior_far, prior),
        (volume_far, volume), (drag_far, drag),
    )
    near = [pltpu.make_async_copy(a, b, near_sem.at[k]) for k, (a, b) in enumerate(pairs)]
    for copy in near:
        copy.start()
    grid = Grid()
    span_size = grid.span_size
    values, _, per, cols = recv.shape
    lines = span_size * per
    part_rows = slab.shape[1]
    width_x, width_y = solid.shape[1:]
    comps = 1 + prior.shape[0]

    barrier = pltpu.get_barrier_semaphore()
    for k in range(1, span_size):
        to = lax.rem(grid.span + k, span_size)
        pl.semaphore_signal(barrier, inc=1, device_id=(to, grid.depth), device_id_type=MESH)
    for dx, dy in Y_STEPS:
        grid.signal(barrier, dx, dy)

    keys = layers * span_size
    live_count = count[0, 0]
    many = wide // block

    def lanes_at(first, size):
        return pl.ds(pl.multiple_of(first, size), size)

    def member_of(first):
        lanes = lanes_at(first, block)
        live = first + lax.broadcasted_iota(jnp.int32, (1, block), 1) < live_count
        layer = lax.shift_right_arithmetic(cell[:, lanes], shift)
        key = jnp.where(live, layer * span_size + slab[:, lanes], -1)
        member = jnp.where(lax.broadcasted_iota(jnp.int32, (keys, block), 0) == key, 1.0, 0.0)
        return member, live

    fold = min(block, LANES)

    def tally(b, total):
        for m in range(many):
            member = member_of(b * wide + m * block)[0]
            for k in range(block // fold):
                total = total + member[:, k * fold : (k + 1) * fold]
        return total

    near[0].wait()
    near[1].wait()
    total = lax.fori_loop(0, part_rows // wide, tally, jnp.zeros((keys, fold), F32))
    near[2].wait()
    near[3].wait()
    for c in range(comps):
        field = solid if c == 0 else prior.at[c - 1]
        for x in range(width_x):
            line = field[:, x, :]
            if x < RIM:
                rows_out[c, 0, x] = line
            if x >= width_x - RIM:
                rows_out[c, 1, x - width_x + RIM] = line
            cols_out[c, 0, x] = line[:, :LANES]
            cols_out[c, 1, x] = line[:, width_y - LANES :]
    for side in range(2):

        @pl.when(jnp.logical_not(grid.has(*X_STEPS[side])))
        def _(side=side):
            rows_in[:, side] = jnp.zeros((comps, RIM, layers, width_y), F32)

        @pl.when(jnp.logical_not(grid.has(*Y_STEPS[side])))
        def _(side=side):
            cols_in[:, side] = jnp.zeros((comps, width_x, layers, LANES), F32)

    def halo_of(at):
        mine = pl.ds(*((0, comps // 2), (comps // 2, comps - comps // 2))[at])
        return Halo(
            grid,
            lambda side: rows_out.at[mine, side],
            lambda side: rows_in.at[mine, side],
            lambda part, side: cols_out.at[mine, side],
            lambda part, side: cols_in.at[mine, side],
            lambda copy: halo_send.at[at, copy],
            lambda copy: halo_recv.at[at, copy],
        )

    halos = [halo_of(at) for at in range(2)]
    pl.semaphore_wait(barrier, span_size - 1 + grid.around(Y_STEPS))
    halos[0].start()

    before_lane = lax.broadcasted_iota(jnp.int32, (block, block), 0)
    this_lane = lax.broadcasted_iota(jnp.int32, (block, block), 1)
    tri = jnp.where(before_lane < this_lane, 1.0, 0.0).astype(BF)
    total = jnp.sum(total, axis=1, keepdims=True)
    counts = [total[k * span_size : (k + 1) * span_size] for k in range(layers)]
    rest = [None] * layers
    left = jnp.zeros((span_size, 1), F32)
    for k in reversed(range(layers)):
        left = left + counts[k]
        rest[k] = left
    base = lax.broadcasted_iota(jnp.int32, (span_size, 1), 0).astype(F32) * cap
    end = jnp.zeros((span_size, 1), F32)
    starts = []
    for k in range(layers):
        start = jnp.minimum(jnp.maximum(end, float(cap // layers * k)), cap - rest[k])
        starts.append(start + base)
        end = start + counts[k]

    def rank(b, offset):
        for m in range(many):
            first = b * wide + m * block
            member, live = member_of(first)
            before = jnp.dot(member.astype(BF), tri, preferred_element_type=F32)
            place = jnp.sum(member * (before + offset), axis=0, keepdims=True).astype(jnp.int32)
            slots[:, lanes_at(first, block)] = jnp.where(live, place, -1)
            offset = offset + jnp.sum(member, axis=1, keepdims=True)
        return offset

    lax.fori_loop(0, part_rows // wide, rank, jnp.concatenate(starts, axis=0))

    near[4].wait()
    near[5].wait()
    groups = ((0, 2), (2, values - 2))

    def own_copy(at):
        mine = pl.ds(*groups[at])
        return pltpu.make_async_copy(
            packed.at[mine, grid.span], recv.at[mine, grid.span], own_sem.at[at]
        )

    def copy_to(at, k):
        mine = pl.ds(*groups[at])
        to = lax.rem(grid.span + k, span_size)
        return pltpu.make_async_remote_copy(
            src_ref=packed.at[mine, to],
            dst_ref=recv.at[mine, grid.span],
            send_sem=send_sem.at[at, k],
            recv_sem=recv_sem.at[at, k],
            device_id=(to, grid.depth),
            device_id_type=MESH,
        )

    for at, (first_value, number) in enumerate(groups):
        mine = pl.ds(first_value, number)

        def place_values(b, carry, first_value=first_value, number=number, mine=mine):
            lanes = lanes_at(b * wide, wide)
            slot = slots[:, lanes]
            row = lax.shift_right_arithmetic(slot, int(math.log2(cols)))
            col = lax.bitwise_and(slot, cols - 1)
            taken = []
            for v in range(first_value, first_value + number):
                if v == 0:
                    taken.append((cell[:, lanes] + 1).astype(F32))
                else:
                    taken.append(volume[:, lanes] if v == 1 else drag[v - 2, :, lanes])
            sums = spread(taken, row, col, lines, cols).reshape(number, span_size, per, cols)
            packed[mine] += sums
            return carry

        packed[mine] = jnp.zeros((number, span_size, per, cols), F32)
        lax.fori_loop(0, part_rows // wide, place_values, 0)
        own_copy(at).start()
        for k in range(1, span_size):
            copy_to(at, k).start()
    halos[1].start()
    near_target[...] = jnp.zeros_like(near_target)
    for at in range(len(groups)):
        own_copy(at).wait()
    if bins.binned:
        batch = math.gcd(span_size, BATCH)

        def batch_step(b, carry):
            owners = []
            for i in range(batch):
                k = b * batch + i

                @pl.when(k > 0)
                def _(k=k):
                    for at in range(len(groups)):
                        copy_to(at, k).wait_recv()

                owners.append(lax.rem(grid.span + span_size - k, span_size))
            near_sums(bins, recv, owners, near_target)
            return carry

        lax.fori_loop(0, span_size // batch, batch_step, 0)
    else:
        for at in range(len(groups)):
            for k in range(1, span_size):
                copy_to(at, k).wait_recv()
    for at in range(len(groups)):
        for k in range(1, span_size):
            copy_to(at, k).wait_send()
    for halo in halos:
        halo.rows_arrive()
        halo.arrive((0,))
        halo.rows_sent()
        halo.cols_sent((0,))


def sweeps_kernel(
    bins, solid_far, prior_far, prior_rows, prior_cols, target, ids_ref, out, early_values,
    solid, prior, near_sem, source, first, second, middle, source_cols, middle_cols, corners, tables, send_sem, recv_sem,
    corner_send, corner_recv,
):
    grid = Grid()
    comps, layers, width_x, width_y = target.shape
    near = [
        pltpu.make_async_copy(a, b, near_sem.at[k])
        for k, (a, b) in enumerate(((solid_far, solid), (prior_far, prior)))
    ]
    for copy in near:
        copy.start()
    total_x = width_x + 2 * RIM
    own = pl.ds(0, width_y)
    rest = pl.ds(width_y, LANES)
    own_rows = pl.ds(RIM, width_x)

    barrier = pltpu.get_barrier_semaphore()
    for dx, dy in X_STEPS + Y_STEPS:
        grid.signal(barrier, dx, dy)

    def halo_of(c, phase):
        buffer, cols_in = (source, source_cols) if phase == 0 else (middle, middle_cols)
        width = RIM - 1 if phase == 0 else RIM

        def rows_out(side):
            return buffer.at[c, pl.ds(RIM if side == 0 else RIM + width_x - width, width), :, own]

        def rows_in(side):
            return buffer.at[c, pl.ds(RIM - width if side == 0 else RIM + width_x, width), :, own]

        def rows_of(part):
            return pl.ds(*((RIM, width_x), (RIM - width, width), (RIM + width_x, width))[part])

        def edge(part, side):
            lanes = pl.ds(0 if side == 0 else width_y - LANES, LANES)
            return buffer.at[c, rows_of(part), :, lanes]

        def columns(part, side):
            return cols_in.at[c, side, rows_of(part)]

        return Halo(
            grid, rows_out, rows_in, edge, columns,
            lambda at: send_sem.at[c, phase, at], lambda at: recv_sem.at[c, phase, at],
        )

    def corner_edge(part, side):
        lanes = pl.ds(0 if side == 0 else width_y - LANES, LANES)
        return prior_rows.at[:, part - 1, :, :, lanes]

    around = Halo(
        grid, None, None, corner_edge, lambda part, side: corners.at[:, side, part - 1],
        lambda at: corner_send.at[at], lambda at: corner_recv.at[at],
    )
    halos = [[halo_of(c, phase) for phase in range(2)] for c in range(comps)]
    lane = lax.broadcasted_iota(jnp.int32, (1, layers, LANES), 2)

    def fill_cols(buffer, c, cols_in):
        buffer[c, :, :, rest] = jnp.where(lane < LANES // 2, cols_in[c, 1], cols_in[c, 0])

    for c in range(comps):
        for x in range(width_x):
            source[c, RIM + x, :, own] = target[c, :, x, :]
    for copy in near:
        copy.wait()
    for c in range(comps):
        field = solid if c == 0 else prior.at[c - 1]
        for x in range(width_x):
            first[c, RIM + x, :, own] = field[:, x, :]
        first[c, pl.ds(0, RIM), :, own] = prior_rows[c, 0]
        first[c, pl.ds(RIM + width_x, RIM), :, own] = prior_rows[c, 1]
        first[c, own_rows, :, rest] = jnp.where(lane < LANES // 2, prior_cols[c, 1], prior_cols[c, 0])

    pl.semaphore_wait(barrier, grid.around(X_STEPS + Y_STEPS))
    for c in range(comps):
        halos[c][0].start()
    around.start_cols((1, 2))
    for side, at in ((0, 0), (1, RIM + width_x)):

        @pl.when(jnp.logical_not(grid.has(*X_STEPS[side])))
        def _(at=at):
            for buffer in (source, middle):
                zeros = jnp.zeros((comps, RIM, layers, width_y), F32)
                buffer[:, pl.ds(at, RIM), :, own] = zeros

        @pl.when(jnp.logical_not(grid.has(*Y_STEPS[side])))
        def _(side=side):
            for buffer in (source_cols, middle_cols):
                buffer[:, side] = jnp.zeros((comps, total_x, layers, LANES), F32)
            corners[:, side] = jnp.zeros((comps, 2, RIM, layers, LANES), F32)

    lanes = lax.broadcasted_iota(jnp.int32, (layers, width_y + LANES), 1)
    known = lanes < width_y
    known = known | ((lanes < width_y + LANES // 2) & (grid.depth < grid.depth_size - 1))
    known = known | ((lanes >= width_y + LANES // 2) & (grid.depth > 0))
    scale = jnp.where(known, 1.0 / (1.0 + 4.0 * NU_WEIGHT), 0.0)

    def relax(c, x, before, here, after):
        beside = before + after
        beside = beside + pltpu.roll(here, 1, 1) + pltpu.roll(here, width_y + LANES - 1, 1)
        return (source[c, x] + NU_WEIGHT * beside) * scale

    def sweep(c, old, new, gone):
        low, high = gone, total_x - gone
        step = max(k for k in range(1, 9) if (high - low) % k == 0)

        def rows(g, carry):
            before, here = carry
            for k in range(step):
                x = low + g * step + k
                after = old[c, x + 1]
                new[c, x] = relax(c, x, before, here, after)
                before, here = here, after
            return before, here

        lax.fori_loop(0, (high - low) // step, rows, (old[c, low - 1], old[c, low]))
        for side, x in ((0, RIM - 1), (1, RIM + width_x)):
            if low <= x < high:

                @pl.when(jnp.logical_not(grid.has(*X_STEPS[side])))
                def _(x=x):
                    new[c, x] = jnp.zeros((layers, width_y + LANES), F32)

    def first_half(c):
        halos[c][0].arrive()
        fill_cols(source, c, source_cols)
        sweep(c, first, second, 1)
        sweep(c, second, first, 2)
        sweep(c, first, middle, 3)
        halos[c][1].start()

    def second_half(c):
        halos[c][1].arrive()
        fill_cols(middle, c, middle_cols)
        sweep(c, middle, first, 1)
        sweep(c, first, second, 2)
        before, here = second[c, RIM - 1], second[c, RIM]
        for x in range(width_x):
            after = second[c, RIM + x + 1]
            out[c, :, x, :] = relax(c, RIM + x, before, here, after)[:, :width_y]
            before, here = here, after

    around.arrive((1, 2))
    for c in range(comps):
        for part, at in ((0, 0), (1, RIM + width_x)):
            first[c, pl.ds(at, RIM), :, rest] = jnp.where(
                lane < LANES // 2, corners[c, 1, part], corners[c, 0, part]
            )
    halos[0][0].forward()
    for c in range(comps):
        if c + 1 < comps:
            halos[c + 1][0].forward()
        else:
            halos[0][1].forward()
        first_half(c)
    early = early_values.shape[0]
    parts = comps - early

    early_values[...] = jnp.zeros_like(early_values)

    def put(c, owner, line, lanes, value):
        early_values[c, owner, pl.ds(line, 1), lanes] = value

    for c in range(comps):
        if c + 1 < comps:
            halos[c + 1][1].forward()
        second_half(c)
        if not bins.binned:
            continue
        if c == early - 1:

            def table_step(layer, carry):
                fill_table(bins, tables.at[layer], fields_of(out, layer, range(early)))
                return carry

            lax.fori_loop(0, layers, table_step, 0)
        if early - 1 <= c < comps - 1:
            at = c - early + 1
            share = layers // (2 * parts)
            lines = range(share * at, share * (at + 1))
            near_values(bins, tables, ids_ref, lines, put)
    for c in range(comps):
        for phase in range(2):
            halos[c][phase].sent()
    around.cols_sent((1, 2))


def feedback_kernel(
    bins, wide, ids_ref, early_values, early_tables, late_tables, strays, slots, out,
    values, table, hots, send_sem, recv_sem, own_sem,
):
    grid = Grid()
    comps, span_size, per, cols = values.shape
    lines = span_size * per
    part_rows = slots.shape[1]
    early = early_values.shape[0]
    barrier = pltpu.get_barrier_semaphore()
    for k in range(1, span_size):
        to = lax.rem(grid.span + k, span_size)
        pl.semaphore_signal(barrier, inc=1, device_id=(to, grid.depth), device_id_type=MESH)

    def put(c, owner, line, lanes, value):
        more = strays[early + c, owner, pl.ds(line, 1), lanes]
        values[early + c, owner, pl.ds(line, 1), lanes] = value + more

    def put_early(c, owner, line, lanes, value):
        more = strays[c, owner, pl.ds(line, 1), lanes]
        values[c, owner, pl.ds(line, 1), lanes] = value + more

    values[pl.ds(0, early)] = early_values[...] + strays[pl.ds(0, early)]
    copies = []

    def send(first, number):
        mine = pl.ds(first, number)
        at = len(copies)
        started = [
            pltpu.make_async_copy(
                values.at[mine, grid.span], table.at[mine, grid.span], own_sem.at[at]
            )
        ]
        for k in range(1, span_size):
            to = lax.rem(grid.span + k, span_size)
            started.append(
                pltpu.make_async_remote_copy(
                    src_ref=values.at[mine, to],
                    dst_ref=table.at[mine, grid.span],
                    send_sem=send_sem.at[at, k],
                    recv_sem=recv_sem.at[at, k],
                    device_id=(to, grid.depth),
                    device_id_type=MESH,
                )
            )
        for copy in started:
            copy.start()
        copies.append((mine, started))

    half = bins.layers // 2
    if bins.binned:
        near_values(bins, early_tables, ids_ref, range(half, bins.layers), put_early)
    else:
        values[pl.ds(early, comps - early)] = strays[pl.ds(early, comps - early)]
    pl.semaphore_wait(barrier, span_size - 1)
    send(0, early)
    if bins.binned:
        near_values(bins, late_tables, ids_ref, range(bins.layers), put)
    send(early, comps - early)

    def lanes_at(b):
        return pl.ds(pl.multiple_of(b * wide, wide), wide)

    def hot_step(b, carry):
        lanes = lanes_at(b)
        hots[:, lanes] = hot_at(lax.bitwise_and(slots[:, lanes], cols - 1), cols)
        return carry

    lax.fori_loop(0, part_rows // wide, hot_step, 0)
    for mine, started in copies:
        for copy in started:
            copy.wait()
        number = mine.size
        high, low = two_parts(table[mine].reshape(number * lines, cols))
        both = jnp.concatenate([high, low], axis=0)

        def pick_step(b, carry, mine=mine, number=number, both=both):
            lanes = lanes_at(b)
            row = lax.shift_right_arithmetic(slots[:, lanes], int(math.log2(cols)))
            wanted = lax.broadcasted_iota(jnp.int32, (lines, wide), 0) == row
            found = jnp.dot(both, hots[:, lanes], preferred_element_type=F32)
            for c in range(number):
                value = found[c * lines : (c + 1) * lines]
                value = value + found[(number + c) * lines : (number + c + 1) * lines]
                value = jnp.sum(jnp.where(wanted, value, 0.0), axis=0, keepdims=True)
                out[mine.start + c, :, lanes] = value
            return carry

        lax.fori_loop(0, part_rows // wide, pick_step, 0)


VMEM = pl.BlockSpec(memory_space=pltpu.VMEM)
SMEM = pl.BlockSpec(memory_space=pltpu.SMEM)
HBM = pl.BlockSpec(memory_space=pltpu.HBM)
LIMIT = pltpu.CompilerParams(vmem_limit_bytes=48 * 1024 * 1024)


def far(number):
    return pltpu.CompilerParams(
        vmem_limit_bytes=48 * 1024 * 1024, collective_id=number, has_side_effects=True
    )


def on_device(part_slab, part_cell, part_volume, part_drag, part_count, prior_solid, prior_drag):
    span_size = lax.axis_size("span")
    part_rows = part_cell.shape[1]
    cap = 2 * part_rows // span_size
    layers, width_x, width_y = prior_solid.shape
    cols = min(256, cap)
    lines = span_size * cap // cols
    per = lines // span_size
    block = math.gcd(part_rows, 512)
    wide = math.gcd(part_rows, 2048)
    total_x = width_x + 2 * RIM
    dma = pltpu.SemaphoreType.DMA
    bins = Bins(layers, width_x, width_y, span_size, lines, cols)
    recv, slots, prior_rows, prior_cols, near_target = pl.pallas_call(
        functools.partial(
            collect_kernel, bins, cap, block, wide, layers, int(math.log2(width_x * width_y))
        ),
        out_shape=(
            jax.ShapeDtypeStruct((5, span_size, per, cols), F32),
            jax.ShapeDtypeStruct((1, part_rows), jnp.int32),
            jax.ShapeDtypeStruct((4, 2, RIM, layers, width_y), F32),
            jax.ShapeDtypeStruct((4, 2, width_x, layers, LANES), F32),
            jax.ShapeDtypeStruct((4, layers, width_x, width_y), F32),
        ),
        in_specs=[SMEM] + [HBM] * 6,
        out_specs=(VMEM,) * 5,
        scratch_shapes=[
            pltpu.VMEM((5, span_size, per, cols), F32),
            pltpu.VMEM((4, 2, RIM, layers, width_y), F32),
            pltpu.VMEM((4, 2, width_x, layers, LANES), F32),
            pltpu.VMEM((1, part_rows), jnp.int32),
            pltpu.VMEM((1, part_rows), jnp.int32),
            pltpu.VMEM((1, part_rows), F32),
            pltpu.VMEM(part_drag.shape, F32),
            pltpu.VMEM(prior_solid.shape, F32),
            pltpu.VMEM(prior_drag.shape, F32),
            dma((2, HALO_COPIES)),
            dma((2, HALO_COPIES)),
            dma((2, span_size)),
            dma((2, span_size)),
            dma((2,)),
            dma((6,)),
        ],
        compiler_params=far(1),
        name="collect",
    )(
        part_count,
        *[
            pltpu.with_memory_space_constraint(a, pltpu.HBM)
            for a in (
                part_slab.reshape(1, part_rows), part_cell, part_volume, part_drag,
                prior_solid, prior_drag,
            )
        ],
    )
    recv = recv.reshape(5, lines, cols)
    target = pl.pallas_call(
        functools.partial(deposit_kernel, bins),
        out_shape=jax.ShapeDtypeStruct((4, layers, width_x, width_y), F32),
        in_specs=[VMEM] * 2,
        out_specs=VMEM,
        compiler_params=LIMIT,
        name="deposit",
    )(near_target, recv)
    whole = pltpu.VMEM((4, total_x, layers, width_y + LANES), F32)
    columns = pltpu.VMEM((4, 2, total_x, layers, LANES), F32)
    slots_of = (span_size, per, cols)
    smooth, early_values = pl.pallas_call(
        functools.partial(sweeps_kernel, bins),
        out_shape=(
            jax.ShapeDtypeStruct(target.shape, F32),
            jax.ShapeDtypeStruct((2, *slots_of), F32),
        ),
        in_specs=[HBM] * 2 + [VMEM] * 4,
        out_specs=(VMEM, VMEM),
        scratch_shapes=[
            pltpu.VMEM(prior_solid.shape, F32),
            pltpu.VMEM(prior_drag.shape, F32),
            dma((2,)),
        ]
        + [whole] * 4
        + [columns] * 2
        + [pltpu.VMEM((4, 2, 2, RIM, layers, LANES), F32)]
        + [pltpu.VMEM((layers, 4 * bins.rows, bins.cols), BF)]
        + [dma((4, 2, HALO_COPIES))] * 2
        + [dma((HALO_COPIES,))] * 2,
        compiler_params=far(0),
        name="sweeps",
    )(
        pltpu.with_memory_space_constraint(prior_solid, pltpu.HBM),
        pltpu.with_memory_space_constraint(prior_drag, pltpu.HBM),
        prior_rows, prior_cols, target, recv,
    )
    fields, early_tables, late_tables, strays = pl.pallas_call(
        functools.partial(fields_kernel, bins),
        out_shape=(
            jax.ShapeDtypeStruct((4, layers, width_x, width_y), F32),
            jax.ShapeDtypeStruct((layers, 4 * bins.rows, bins.cols), BF),
            jax.ShapeDtypeStruct((layers, 4 * bins.rows, bins.cols), BF),
            jax.ShapeDtypeStruct((4, lines, cols), F32),
        ),
        in_specs=[VMEM] * 2,
        out_specs=(VMEM,) * 4,
        scratch_shapes=[pltpu.VMEM((layers, 8 * bins.rows, bins.cols), BF)],
        compiler_params=LIMIT,
        name="fields",
    )(smooth, recv)
    feedback = pl.pallas_call(
        functools.partial(feedback_kernel, bins, wide),
        out_shape=jax.ShapeDtypeStruct((4, 1, part_rows), F32),
        in_specs=[VMEM] * 6,
        out_specs=VMEM,
        scratch_shapes=[
            pltpu.VMEM((4, *slots_of), F32),
            pltpu.VMEM((4, *slots_of), F32),
            pltpu.VMEM((cols, part_rows), BF),
            dma((2, span_size)),
            dma((2, span_size)),
            dma((2,)),
        ],
        compiler_params=far(2),
        name="feedback",
    )(recv, early_values, early_tables, late_tables, strays.reshape(4, *slots_of), slots)
    return (fields, feedback)


def solution(mesh):
    in_specs = (
        P("depth", "span", None),
        P("depth", "span"),
        P("depth", "span"),
        P(None, "depth", "span"),
        P("depth", "span"),
        P(None, "span", "depth"),
        P(None, None, "span", "depth"),
    )
    out_specs = (P(None, None, "span", "depth"), P(None, "depth", "span"))
    return jax.shard_map(
        on_device, mesh=mesh, in_specs=in_specs, out_specs=out_specs, check_vma=False
    )
```
